32 devices in a mesh: seq: 4 (over y, core), tp: 8 (over z, x).
Axes of the slice: x: 2, y: 2, z: 4, core: 2. Of those that a mesh axis runs over, the one named last changes fastest.
Arguments:
- tokens: bfloat16 [2048, 4608], P(('seq', 'tp')), may hold values from -6 to 6
- norm_gain: float32 [4608], replicated, may hold values from 0.1 to 1.9
- query_weight: bfloat16 [4608, 4096], P(None, 'tp'), may hold values from -6 to 6
- key_matrix: bfloat16 [4608, 2048], P(None, 'tp'), may hold values from -0.09375 to 0.09375
- value_matrix: bfloat16 [4608, 2048], P(None, 'tp'), may hold values from -0.09375 to 0.09375
- output_grad: bfloat16 [2048, 4096], P('seq', 'tp'), may hold values from -3 to 3
Outputs:
- input_gradient: bfloat16 [2048, 4608], P(('seq', 'tp'))
The draws below stay inside these ranges and needn't reach their ends.
All inputs are finite; a program needn't handle non-finite values.
Results may differ from the reference program's by a relative error of at most 0.014.
The reference program's roundings to bfloat16 on the way (of `normed` and `grad_query`) count: a program that leaves them out, or rounds other values in their place, can miss the bound.
Values may be sent and summed in bfloat16 or wider, within the bound.
A program may use at most 64 MiB of HBM per device.

```python
import math
import jax
import jax.numpy as jnp
from jax import lax

MODEL_WIDTH = 4608
HQ = 32
KEY_VALUE_HEADS = 16
HEAD_SIZE = 128
TOK_DEV = 512
WINDOW = 640
TOKENS = 2048


def draw_query_weight(key, part):
    head_scale = jnp.exp(jax.random.uniform(jax.random.fold_in(key, 11), (HQ,), jnp.float32, math.log(3.0), math.log(12.0)))
    column_scale = jnp.repeat(head_scale, HEAD_SIZE)
    entries = jax.random.truncated_normal(jax.random.fold_in(key, 12), -4.0, 4.0, (MODEL_WIDTH, HQ * HEAD_SIZE), jnp.float32)
    return (entries * column_scale[None, :] / math.sqrt(MODEL_WIDTH)).astype(jnp.bfloat16)


def strengthened(values, stream_key, source, target, blocks, factor):
    def block_of(axis_at):
        return (jnp.arange(values.shape[axis_at]) // (values.shape[axis_at] // blocks)).reshape((-1,) + (1,) * (values.ndim - 1 - axis_at))

    near = jax.random.permutation(stream_key, blocks)[block_of(target)]
    far = (block_of(target) + blocks // 2) % blocks
    return jnp.where((block_of(source) == near) | (block_of(source) == far), factor * values, values)


def block_scale(own_key, extent, pieces, smallest, top_value):
    gain = 1.0
    for axis_at, shards_of in pieces:
        steps = jax.random.uniform(jax.random.fold_in(jax.random.fold_in(own_key, 6), axis_at), (shards_of,), jnp.float32, smallest / len(pieces), top_value / len(pieces))
        gain = gain * jnp.repeat(jnp.exp(steps), extent[axis_at] // shards_of).reshape((-1,) + (1,) * (len(extent) - 1 - axis_at))
    return gain


def gaussian(own_key, shape, width, reach, split=(), kind=jnp.bfloat16):
    values = jax.random.normal(own_key, shape, jnp.float32) * width
    if len(split) > 0:
        values = block_scale(own_key, shape, split, -0.22, 0.18) * values
    return jnp.clip(values, min=-reach, max=reach).astype(kind)


def bell_draw_with(own_key, shape, width, bound, shards, heavy, held_as=jnp.bfloat16):
    result = width * jax.random.normal(own_key, shape, jnp.float32)
    if shards:
        result = result * block_scale(own_key, shape, shards, -0.22, 0.18)
    return jnp.clip(strengthened(result, jax.random.fold_in(own_key, 3), *heavy), -bound, bound).astype(held_as)


def setup_inputs(seed: int = 0) -> dict:
    key_of = jax.random.split(jax.random.key(seed), 7)
    tokens = gaussian(key_of[0], (TOKENS, MODEL_WIDTH), 1.0, 6.0, ((0, 32),))
    norm_gain = jnp.clip(1.0 + 0.18 * jax.random.normal(key_of[1], (MODEL_WIDTH,), jnp.float32), 0.1, 1.9)
    query_weight = draw_query_weight(jax.random.fold_in(key_of[6], 71), 0)
    key_matrix = gaussian(key_of[3], (MODEL_WIDTH, KEY_VALUE_HEADS * HEAD_SIZE), MODEL_WIDTH ** -0.5, 0.09375, ((1, 8),))
    value_matrix = gaussian(key_of[4], (MODEL_WIDTH, KEY_VALUE_HEADS * HEAD_SIZE), MODEL_WIDTH ** -0.5, 0.09375, ((1, 8),))
    output_grad = bell_draw_with(key_of[5], (TOKENS, HQ * HEAD_SIZE), 0.5, 3.0, ((0, 4), (1, 8)), (1, 0, 8, 2.0))
    return dict(tokens=tokens, norm_gain=norm_gain, query_weight=query_weight, key_matrix=key_matrix, value_matrix=value_matrix, output_grad=output_grad)


SCALE = 1.0 / 12.0
CAP = 50.0
EPS = 1e-06

def block_grads(query_blk, grad_blk, key_blk, value_blk, query_pos, key_pos):
    row_count = query_blk.shape[0]
    key_span = key_blk.shape[0]
    kv_heads = key_blk.shape[1] // HEAD_SIZE
    groups = query_blk.shape[1] // key_blk.shape[1]
    query_four = query_blk.reshape(row_count, kv_heads, groups, HEAD_SIZE).astype(jnp.float32)
    grad_four = grad_blk.reshape(row_count, kv_heads, groups, HEAD_SIZE).astype(jnp.float32)
    key_three = key_blk.reshape(key_span, kv_heads, HEAD_SIZE).astype(jnp.float32)
    value_three = value_blk.reshape(key_span, kv_heads, HEAD_SIZE).astype(jnp.float32)
    raw = jnp.einsum('qkgd,skd->kgqs', query_four, key_three)
    bent = jnp.tanh(raw * SCALE / CAP)
    capped = CAP * bent
    valid = (key_pos[None, :] <= query_pos[:, None]) & (key_pos[None, :] > query_pos[:, None] - WINDOW) & (key_pos[None, :] >= 0)
    expo = jnp.where(valid, jnp.exp(capped), 0.0)
    probs = expo / lax.optimization_barrier(jnp.sum(expo, axis=-1, keepdims=True))
    d_probs = jnp.einsum('qkgd,skd->kgqs', grad_four, value_three)
    delta = lax.optimization_barrier(jnp.sum(probs * d_probs, axis=-1, keepdims=True))
    d_raw = (probs * (d_probs - delta) * (1.0 - bent * bent) * SCALE).astype(jnp.bfloat16).astype(jnp.float32)
    probs_low = probs.astype(jnp.bfloat16).astype(jnp.float32)
    grad_query = jnp.einsum('kgqs,skd->qkgd', d_raw, key_three).reshape(row_count, kv_heads * groups * HEAD_SIZE)
    grad_key = jnp.einsum('kgqs,qkgd->skd', d_raw, query_four).reshape(key_span, kv_heads * HEAD_SIZE)
    grad_value = jnp.einsum('kgqs,qkgd->skd', probs_low, grad_four).reshape(key_span, kv_heads * HEAD_SIZE)
    return (grad_query, grad_key, grad_value)

def reference(tokens, norm_gain, query_weight, key_matrix, value_matrix, output_grad):
    total_rows = tokens.shape[0]
    key_cols = key_matrix.shape[1]
    block_rows = min(512, TOK_DEV)
    key_span = WINDOW + block_rows
    float_values = tokens.astype(jnp.float32)
    reciprocal_root_mean = lax.rsqrt(lax.optimization_barrier(jnp.mean(float_values * float_values, axis=1, keepdims=True)) + EPS)
    normed = (float_values * reciprocal_root_mean * norm_gain).astype(jnp.bfloat16)
    query_all = jnp.dot(normed, query_weight, preferred_element_type=jnp.float32).astype(jnp.bfloat16)
    key_all = jnp.dot(normed, key_matrix, preferred_element_type=jnp.float32).astype(jnp.bfloat16)
    value_all = jnp.dot(normed, value_matrix, preferred_element_type=jnp.float32).astype(jnp.bfloat16)
    pad_key = jnp.concatenate([jnp.zeros((WINDOW, key_cols), jnp.bfloat16), key_all], axis=0)
    pad_value = jnp.concatenate([jnp.zeros((WINDOW, key_cols), jnp.bfloat16), value_all], axis=0)

    def step_fn(carry, index_block):
        acc_key, acc_value = carry
        first_row = index_block * block_rows
        query_blk = lax.dynamic_slice_in_dim(query_all, first_row, block_rows, 0)
        grad_blk = lax.dynamic_slice_in_dim(output_grad, first_row, block_rows, 0)
        key_blk = lax.dynamic_slice_in_dim(pad_key, first_row, key_span, 0)
        value_blk = lax.dynamic_slice_in_dim(pad_value, first_row, key_span, 0)
        query_pos = first_row + jnp.arange(block_rows, dtype=jnp.int32)
        key_pos = first_row - WINDOW + jnp.arange(key_span, dtype=jnp.int32)
        grad_query, grad_key, grad_value = block_grads(query_blk, grad_blk, key_blk, value_blk, query_pos, key_pos)
        acc_key = lax.dynamic_update_slice_in_dim(acc_key, lax.dynamic_slice_in_dim(acc_key, first_row, key_span, 0) + grad_key, first_row, 0)
        acc_value = lax.dynamic_update_slice_in_dim(acc_value, lax.dynamic_slice_in_dim(acc_value, first_row, key_span, 0) + grad_value, first_row, 0)
        return ((acc_key, acc_value), grad_query.astype(jnp.bfloat16))
    zeros_acc = jnp.zeros((total_rows + WINDOW, key_cols), jnp.float32)
    (acc_key, acc_value), grad_blocks = lax.scan(step_fn, (zeros_acc, zeros_acc), jnp.arange(total_rows // block_rows, dtype=jnp.int32))
    grad_query = grad_blocks.reshape(total_rows, query_weight.shape[1])
    grad_key = acc_key[WINDOW:].astype(jnp.bfloat16)
    grad_value = acc_value[WINDOW:].astype(jnp.bfloat16)
    dims = (((1,), (1,)), ((), ()))
    d_norm = lax.dot_general(grad_query, query_weight, dims, preferred_element_type=jnp.float32)
    d_norm = d_norm + lax.dot_general(grad_key, key_matrix, dims, preferred_element_type=jnp.float32)
    d_norm = d_norm + lax.dot_general(grad_value, value_matrix, dims, preferred_element_type=jnp.float32)
    upper_limit = d_norm * norm_gain
    normalized_input = float_values * reciprocal_root_mean
    input_gradient = reciprocal_root_mean * (upper_limit - normalized_input * lax.optimization_barrier(jnp.mean(upper_limit * normalized_input, axis=1, keepdims=True)))
    return input_gradient.astype(jnp.bfloat16)
```

```python
import functools
import types

import jax
import jax.numpy as jnp
from jax import lax
from jax.experimental import pallas as pl
from jax.experimental.pallas import tpu as pltpu
from jax.sharding import PartitionSpec as P

HEAD_SIZE = 128
WINDOW = 640


SCALE = 1.0 / 12.0
CAP = 50.0
EPS = 1e-06
VMEM_BYTES = 60 * 1024 * 1024
QUERY_ROWS = 128
KEY_TILE = 256
LOG2E = 1.4426950408889634
TILE = 256


def ring_place(index, n):
    odd = index % 2
    return (1 - odd) * (index // 2) + odd * (n - 1 - index // 2)


def ring_device(place, n):
    place = (place + n) % n
    late = place // (n // 2)
    return (1 - late) * 2 * place + late * (2 * (n - 1 - place) + 1)


def chunks_of(direction, hop, last):
    return (direction, 1 - direction) if hop < last else (direction,)


def greet(neighbours):
    barrier = pltpu.get_barrier_semaphore()
    for neighbour in neighbours:
        pl.semaphore_signal(
            barrier, inc=1, device_id=neighbour, device_id_type=pl.DeviceIdType.MESH
        )


def hear(neighbours):
    pl.semaphore_wait(pltpu.get_barrier_semaphore(), len(neighbours))


def when(needed, act):
    if needed is None:
        act()
    else:
        pl.when(needed)(act)


def remote(source, target, send_sem, recv_sem, device):
    return pltpu.make_async_remote_copy(
        src_ref=source,
        dst_ref=target,
        send_sem=send_sem,
        recv_sem=recv_sem,
        device_id=device,
        device_id_type=pl.DeviceIdType.MESH,
    )


def load_weights(weights, held, sems):
    copies = []
    start = 0
    for i, weight in enumerate(weights):
        cols = weight.shape[1]
        copies.append(
            pltpu.make_async_copy(weight, held.at[:, start : start + cols], sems.at[i])
        )
        start += cols
    return copies


def rows_at(index, count):
    return pl.ds(pl.multiple_of(index * count, count), count)


def gather_phase(n, ring, onward, tokens, gain, loads, s):
    rows, _ = tokens.shape
    local = n * rows
    half = rows // 2
    last = n // 2
    query_cols = s.query.shape[1]
    pair_cols = s.pairs.shape[1]
    me = lax.axis_index("tp")
    place = ring_place(me, n)
    sends = []
    halos = []

    def sender(direction, hop, chunk):
        step = -(hop - 1) if direction == 0 else hop - 1
        owner = ring_device(place + step, n)
        part = pl.ds(chunk * half, half)
        return remote(
            tokens.at[part] if hop == 1 else s.gathered.at[owner, part],
            s.gathered.at[owner, part],
            s.gather_send.at[direction, hop - 1, chunk],
            s.gather_recv.at[direction, hop - 1, chunk],
            ring[direction],
        )

    def project(sources):
        for i, (block, _) in enumerate(sources):
            values = block[...].astype(jnp.float32)
            scale = lax.rsqrt(jnp.mean(values * values, axis=1, keepdims=True) + EPS)
            s.normed[i * rows : (i + 1) * rows] = (values * scale * gain[...]).astype(jnp.bfloat16)
        count = len(sources) * rows

        def column(target, base, first):
            def write(j, carry):
                product = jnp.dot(
                    s.normed[:count],
                    s.held[:, pl.ds(pl.multiple_of(first + j * TILE, TILE), TILE)],
                    preferred_element_type=jnp.float32,
                ).astype(jnp.bfloat16)
                for i, (_, owner) in enumerate(sources):
                    at = pl.ds(pl.multiple_of(base + owner * rows, rows), rows)
                    target[at, rows_at(j, TILE)] = product[i * rows : (i + 1) * rows]
                return carry

            return write

        lax.fori_loop(0, pair_cols // TILE, column(s.pairs, 2 * local, query_cols), 0)
        for _, owner in sources:
            for back in range(2):
                source = pl.ds(pl.multiple_of(2 * local + owner * rows, rows), rows)
                target = pl.ds(pl.multiple_of((1 - back) * local + owner * rows, rows), rows)
                copy = remote(
                    s.pairs.at[source],
                    s.pairs.at[target],
                    s.halo_send.at[back, len(halos) // 2],
                    s.halo_recv.at[back, len(halos) // 2],
                    onward[back],
                )
                needed = (owner + 1) * rows > 2 * local - WINDOW if back else None
                halos.append((copy, needed))
                when(needed, copy.start)
        lax.fori_loop(0, query_cols // TILE, column(s.query, 0, 0), 0)

    for position in range(2):
        for direction in range(2):
            order = chunks_of(direction, 1, last)
            if position < len(order):
                sends.append(sender(direction, 1, order[position]))
                sends[-1].start()
    for copy in loads:
        copy.wait()
    gain[...] = s.gain_flat[...].reshape(gain.shape)
    project([(tokens, me)])
    for hop in range(1, last + 1):
        for position in range(2):
            for direction in range(2):
                order = chunks_of(direction, hop, last)
                if position < len(order):
                    chunk = order[position]
                    sender(direction, hop, chunk).wait_recv()
                    if hop < last and chunk in chunks_of(direction, hop + 1, last):
                        sends.append(sender(direction, hop + 1, chunk))
                        sends[-1].start()
        owners = [ring_device(place - hop, n)]
        if hop < last:
            owners.append(ring_device(place + hop, n))
        project([(s.gathered.at[owner], owner) for owner in owners])
    for copy, needed in halos:
        when(needed, copy.wait_recv)
    return [(copy, None) for copy in sends] + halos


def dot(lhs, rhs, left, right):
    return lax.dot_general(
        lhs, rhs, (((left,), (right,)), ((), ())), preferred_element_type=jnp.float32
    )


def attention_phase(backward, output_grad, s, meanwhile):
    local, query_cols = s.query.shape
    key_cols = s.pairs.shape[1] // 2
    kv_heads = key_cols // HEAD_SIZE
    groups = query_cols // key_cols
    reach = WINDOW - local
    span = WINDOW + QUERY_ROWS
    start = 2 * local - WINDOW
    anchor = lax.axis_index("seq") * local
    shape = (QUERY_ROWS, groups * QUERY_ROWS)
    s.gap[...] = lax.broadcasted_iota(jnp.int32, shape, 0) - (
        lax.broadcasted_iota(jnp.int32, shape, 1) % QUERY_ROWS
    )
    s.sums[...] = jnp.zeros_like(s.sums)
    sends = []

    count = local // QUERY_ROWS
    late = (count - 1) * QUERY_ROWS

    def halo(head, piece, rows):
        part = pl.ds(pl.multiple_of(piece * QUERY_ROWS, QUERY_ROWS), rows)
        return remote(
            s.leaving.at[head, part],
            s.arriving.at[head, part],
            s.back_send.at[head, piece],
            s.back_recv.at[head, piece],
            backward,
        )

    def send_back(head, piece, rows):
        part = pl.ds(pl.multiple_of(piece * QUERY_ROWS, QUERY_ROWS), rows)
        s.leaving[head, part] = s.sums[head, part].astype(jnp.bfloat16)
        halo(head, piece, rows).start()

    def lanes_of(head):
        return [
            slice((head * groups + g) * HEAD_SIZE, (head * groups + g + 1) * HEAD_SIZE)
            for g in range(groups)
        ]

    def rows_of(ref, head, i):
        own = slice(i * QUERY_ROWS, (i + 1) * QUERY_ROWS)
        return jnp.concatenate([ref[own, lanes] for lanes in lanes_of(head)], axis=0)

    def seen_by(head, i, tile, base):
        rows = slice(start + i * QUERY_ROWS + tile, start + i * QUERY_ROWS + tile + KEY_TILE)
        return s.pairs[rows, base + head * HEAD_SIZE : base + (head + 1) * HEAD_SIZE]

    def scores(head, i, slot):
        query = rows_of(s.query, head, i)
        grad = rows_of(output_grad, head, i)
        first = WINDOW - anchor - i * QUERY_ROWS
        total = jnp.zeros((8, shape[1]), jnp.float32)
        along = jnp.zeros((8, shape[1]), jnp.float32)
        for tile in range(0, span, KEY_TILE):
            bent_tile = jnp.tanh(dot(seen_by(head, i, tile, 0), query, 1, 1) * (SCALE / CAP))
            d_tile = dot(seen_by(head, i, tile, key_cols), grad, 1, 1)
            for part in range(0, KEY_TILE, QUERY_ROWS):
                row = tile + part
                bent = bent_tile[part : part + QUERY_ROWS]
                d_probs = d_tile[part : part + QUERY_ROWS]
                expo = jnp.exp2(bent * (CAP * LOG2E))
                if row == 0:
                    expo = jnp.where(s.gap[...] > jnp.where(first > 0, QUERY_ROWS, 0), expo, 0.0)
                elif row < WINDOW:
                    expo = expo * jnp.where(first > row, 0.0, 1.0)
                else:
                    expo = jnp.where(s.gap[...] <= 0, expo, 0.0)
                total += jnp.sum(expo.reshape(-1, 8, shape[1]), axis=0)
                along += jnp.sum((expo * d_probs).reshape(-1, 8, shape[1]), axis=0)
                at = slice(row, row + QUERY_ROWS)
                s.expo[slot, at] = expo.astype(jnp.bfloat16)
                s.slope[slot, at] = expo * (1.0 - bent * bent)
                s.d_probs[slot, at] = d_probs
        inverse = 1.0 / jnp.sum(total, axis=0, keepdims=True)
        delta = jnp.sum(along, axis=0, keepdims=True) * inverse
        column = jnp.transpose(jnp.broadcast_to(inverse, shape))
        return inverse, delta, column

    def gradients(head, i, slot, inverse, delta, column):
        query = (rows_of(s.query, head, i).astype(jnp.float32) * (column * SCALE)).astype(jnp.bfloat16)
        grad = (rows_of(output_grad, head, i).astype(jnp.float32) * column).astype(jnp.bfloat16)
        grad_query = jnp.zeros((shape[1], HEAD_SIZE), jnp.float32)
        for tile in range(0, span, KEY_TILE):
            rows = slice(tile, tile + KEY_TILE)
            d_raw = (s.slope[slot, rows] * (s.d_probs[slot, rows] - delta)).astype(jnp.bfloat16)
            at = slice(i * QUERY_ROWS + tile, i * QUERY_ROWS + tile + KEY_TILE)
            s.sums[head, at, :HEAD_SIZE] += dot(d_raw, query, 1, 0)
            s.sums[head, at, HEAD_SIZE:] += dot(s.expo[slot, rows], grad, 1, 0)
            grad_query += dot(d_raw, seen_by(head, i, tile, 0), 0, 0)
        grad_query = (grad_query * (column * SCALE)).astype(jnp.bfloat16)
        for g, lanes in enumerate(lanes_of(head)):
            s.grads[i * QUERY_ROWS : (i + 1) * QUERY_ROWS, lanes] = grad_query[
                g * QUERY_ROWS : (g + 1) * QUERY_ROWS
            ]

    pieces = [(piece, QUERY_ROWS) for piece in range(count - 1)] + [(count - 1, WINDOW - late)]
    steps = [(head, i) for head in range(kv_heads) for i in range(count)]
    ready = scores(*steps[0], 0)
    for k, (head, i) in enumerate(steps):
        now = ready
        if k + 1 < len(steps):
            ready = scores(*steps[k + 1], (k + 1) % 2)
        gradients(head, i, k % 2, *now)
        if i + 1 == count:
            halo(head, 0, QUERY_ROWS).wait_recv()
            s.sums[head, local:WINDOW] += s.arriving[head, :reach].astype(jnp.float32)
        send_back(head, *pieces[i])
        sends.append((halo(head, *pieces[i]), None))
    meanwhile()
    for head in range(kv_heads):
        for piece in pieces[1:]:
            halo(head, *piece).wait_recv()
        s.sums[head, WINDOW:] += s.arriving[head, reach:].astype(jnp.float32)
        for side in range(2):
            lanes = slice(side * HEAD_SIZE, (side + 1) * HEAD_SIZE)
            column = query_cols + side * key_cols + head * HEAD_SIZE
            s.grads[:, column : column + HEAD_SIZE] = s.sums[head, WINDOW:, lanes].astype(
                jnp.bfloat16
            )
    return sends


def farthest_query_sums(n, rows, s):
    query_cols = s.query.shape[1]
    place = ring_place(lax.axis_index("tp"), n)
    s.picked[:rows, :query_cols] = s.grads[
        rows_at(ring_device(place + n // 2, n), rows), :query_cols
    ]

    def column(j, carry):
        at = rows_at(j, TILE)
        s.total[:rows, at] = dot(s.picked[:rows, :query_cols], s.held[at, :query_cols], 1, 1)
        return carry

    lax.fori_loop(0, s.total.shape[1] // TILE, column, 0)


def scatter_phase(n, ring, tokens, gain, out, s):
    rows, width = tokens.shape
    half = rows // 2
    last = n // 2
    split = width // 2
    query_cols = s.query.shape[1]
    me = lax.axis_index("tp")
    place = ring_place(me, n)

    def sender(direction, hop, chunk):
        part = pl.ds(chunk * half, half)
        return remote(
            s.outgoing.at[direction, hop - 1, part],
            s.incoming.at[direction, hop - 1, part],
            s.scatter_send.at[direction, hop - 1, chunk],
            s.scatter_recv.at[direction, hop - 1, chunk],
            ring[direction],
        )

    def far_sender(direction, side):
        part = pl.ds(direction * half, half)
        lanes = pl.ds(side * split, split)
        return remote(
            s.outgoing.at[direction, last - 1, part, lanes],
            s.incoming.at[direction, last - 1, part, lanes],
            s.scatter_send.at[direction, last - 1, side],
            s.scatter_recv.at[direction, last - 1, side],
            ring[direction],
        )

    def partial_sums(owners):
        for i, owner in enumerate(owners):
            s.picked[i * rows : (i + 1) * rows] = s.grads[rows_at(owner, rows)]
        count = len(owners) * rows

        def column(j, carry):
            at = rows_at(j, TILE)
            s.total[:count, at] = dot(s.picked[:count], s.held[at, :], 1, 1)
            return carry

        lax.fori_loop(0, width // TILE, column, 0)

    def arrivals(direction, hop, chunk):
        if hop < last:
            sender(direction, hop, chunk).wait_recv()
        else:
            for side in range(2):
                far_sender(direction, side).wait_recv()

    sends = []
    s.picked[:rows] = s.grads[rows_at(ring_device(place + last, n), rows)]
    for side in range(2):

        def add_pairs(j, carry):
            at = rows_at(j, TILE)
            s.total[:rows, at] += dot(
                s.picked[:rows, query_cols:], s.held[at, query_cols:], 1, 1
            )
            return carry

        tiles = split // TILE
        lax.fori_loop(side * tiles, (side + 1) * tiles, add_pairs, 0)
        lanes = slice(side * split, (side + 1) * split)
        for direction in range(2):
            part = slice(direction * half, (direction + 1) * half)
            s.outgoing[direction, last - 1, part, lanes] = s.total[part, lanes].astype(jnp.bfloat16)
            sends.append(far_sender(direction, side))
            sends[-1].start()
    for hop in range(last - 1, 0, -1):
        partial_sums([ring_device(place + hop, n), ring_device(place - hop, n)])
        for position in (1, 0):
            for direction in range(2):
                order = chunks_of(direction, hop, last)
                if position < len(order):
                    chunk = order[position]
                    base = direction * rows
                    part = slice(chunk * half, (chunk + 1) * half)
                    value = s.total[base + chunk * half : base + (chunk + 1) * half]
                    if chunk in chunks_of(direction, hop + 1, last):
                        arrivals(direction, hop + 1, chunk)
                        value = value + s.incoming[direction, hop, part].astype(jnp.float32)
                    s.outgoing[direction, hop - 1, part] = value.astype(jnp.bfloat16)
                    sends.append(sender(direction, hop, chunk))
                    sends[-1].start()
    partial_sums([me])
    for chunk in (1, 0):
        part = slice(chunk * half, (chunk + 1) * half)
        value = s.total[part]
        for direction in range(2):
            if chunk in chunks_of(direction, 1, last):
                arrivals(direction, 1, chunk)
                value = value + s.incoming[direction, 0, part].astype(jnp.float32)
        values = tokens[part].astype(jnp.float32)
        scale = lax.rsqrt(jnp.mean(values * values, axis=1, keepdims=True) + EPS)
        upper = value * gain[...]
        unit = values * scale
        out[part] = (
            scale * (upper - unit * jnp.mean(upper * unit, axis=1, keepdims=True))
        ).astype(jnp.bfloat16)
    return sends


def kernel(names, n, seqs, tokens_ref, gain_ref, grad_ref, wq, wk, wv, out, *scratch):
    s = types.SimpleNamespace(**dict(zip(names, scratch)))
    place = ring_place(lax.axis_index("tp"), n)
    block = lax.axis_index("seq")
    ring = [{"tp": ring_device(place + step, n)} for step in (1, -1)]
    onward = [{"seq": (block + step) % seqs} for step in (1, 2)]
    backward = [{"seq": (block + seqs - step) % seqs} for step in (1, 2)]
    greet(ring + onward + backward)
    tokens = s.tokens
    load = pltpu.make_async_copy(tokens_ref, tokens, s.load_sems.at[3])
    loads = load_weights((wq, wk, wv), s.held, s.load_sems)
    loads.append(pltpu.make_async_copy(gain_ref, s.gain_flat, s.load_sems.at[4]))
    loads.append(pltpu.make_async_copy(grad_ref, s.output_grad, s.load_sems.at[5]))
    for copy in [load] + loads:
        copy.start()
    load.wait()
    hear(ring + onward + backward)
    sends = gather_phase(n, ring, onward, tokens, s.gain, loads, s)
    meanwhile = functools.partial(farthest_query_sums, n, tokens.shape[0], s)
    sends += attention_phase(backward[0], s.output_grad, s, meanwhile)
    sends += [(copy, None) for copy in scatter_phase(n, ring, tokens, s.gain, out, s)]
    for copy, needed in sends:
        when(needed, copy.wait_send)


def on_device(tokens, norm_gain, query_weight, key_matrix, value_matrix, output_grad):
    n = lax.axis_size("tp")
    rows, width = tokens.shape
    local, query_cols = output_grad.shape
    key_cols = key_matrix.shape[1]
    cols = query_cols + 2 * key_cols
    kv_heads = key_cols // HEAD_SIZE
    groups = query_cols // key_cols
    low, full = jnp.bfloat16, jnp.float32
    hops = pltpu.SemaphoreType.DMA((2, n // 2, 2))
    blocks = pltpu.SemaphoreType.DMA((2, n))
    heads = pltpu.SemaphoreType.DMA((kv_heads, local // QUERY_ROWS))
    scratch = dict(
        tokens=pltpu.VMEM((rows, width), low),
        output_grad=pltpu.VMEM((local, query_cols), low),
        gain_flat=pltpu.VMEM((width,), full),
        gain=pltpu.VMEM((1, width), full),
        gathered=pltpu.VMEM((n, rows, width), low),
        held=pltpu.VMEM((width, cols), low),
        normed=pltpu.VMEM((2 * rows, width), low),
        query=pltpu.VMEM((local, query_cols), low),
        pairs=pltpu.VMEM((3 * local, 2 * key_cols), low),
        gap=pltpu.VMEM((QUERY_ROWS, groups * QUERY_ROWS), jnp.int32),
        expo=pltpu.VMEM((2, WINDOW + QUERY_ROWS, groups * QUERY_ROWS), low),
        slope=pltpu.VMEM((2, WINDOW + QUERY_ROWS, groups * QUERY_ROWS), full),
        d_probs=pltpu.VMEM((2, WINDOW + QUERY_ROWS, groups * QUERY_ROWS), full),
        sums=pltpu.VMEM((kv_heads, WINDOW + local, 2 * HEAD_SIZE), full),
        leaving=pltpu.VMEM((kv_heads, WINDOW, 2 * HEAD_SIZE), low),
        arriving=pltpu.VMEM((kv_heads, WINDOW, 2 * HEAD_SIZE), low),
        grads=pltpu.VMEM((local, cols), low),
        outgoing=pltpu.VMEM((2, n // 2, rows, width), low),
        incoming=pltpu.VMEM((2, n // 2, rows, width), low),
        picked=pltpu.VMEM((2 * rows, cols), low),
        total=pltpu.VMEM((2 * rows, width), full),
        gather_send=hops,
        gather_recv=hops,
        halo_send=blocks,
        halo_recv=blocks,
        back_send=heads,
        back_recv=heads,
        scatter_send=hops,
        scatter_recv=hops,
        load_sems=pltpu.SemaphoreType.DMA((6,)),
    )
    vmem = pl.BlockSpec(memory_space=pltpu.VMEM)
    hbm = pl.BlockSpec(memory_space=pl.ANY)
    return pl.pallas_call(
        functools.partial(kernel, tuple(scratch), n, lax.axis_size("seq")),
        out_shape=pltpu.VMEM((rows, width), low),
        in_specs=[hbm] * 6,
        out_specs=vmem,
        scratch_shapes=list(scratch.values()),
        compiler_params=pltpu.CompilerParams(
            collective_id=0, has_side_effects=True, vmem_limit_bytes=VMEM_BYTES
        ),
        name="attention_backward",
    )(tokens, norm_gain, output_grad, query_weight, key_matrix, value_matrix)


def solution(mesh):
    return jax.shard_map(
        on_device,
        mesh=mesh,
        in_specs=(
            P(("seq", "tp"), None),
            P(),
            P(None, "tp"),
            P(None, "tp"),
            P(None, "tp"),
            P("seq", "tp"),
        ),
        out_specs=P(("seq", "tp"), None),
        check_vma=False,
    )
```

```python
import functools
import types

import jax
import jax.numpy as jnp
from jax import lax
from jax.experimental import pallas as pl
from jax.experimental.pallas import tpu as pltpu
from jax.sharding import PartitionSpec as P

HEAD_SIZE = 128
WINDOW = 640


SCALE = 1.0 / 12.0
CAP = 50.0
EPS = 1e-06
VMEM_BYTES = 60 * 1024 * 1024
QUERY_ROWS = 128
KEY_TILE = 256
PIECES = 6
LOG2E = 1.4426950408889634
TILE = 256


def ring_place(index, n):
    odd = index % 2
    return (1 - odd) * (index // 2) + odd * (n - 1 - index // 2)


def ring_device(place, n):
    place = (place + n) % n
    late = place // (n // 2)
    return (1 - late) * 2 * place + late * (2 * (n - 1 - place) + 1)


def chunks_of(direction, hop, last):
    return (direction, 1 - direction) if hop < last else (direction,)


def greet(neighbours):
    barrier = pltpu.get_barrier_semaphore()
    for neighbour in neighbours:
        pl.semaphore_signal(
            barrier, inc=1, device_id=neighbour, device_id_type=pl.DeviceIdType.MESH
        )


def hear(neighbours):
    pl.semaphore_wait(pltpu.get_barrier_semaphore(), len(neighbours))


def when(needed, act):
    if needed is None:
        act()
    else:
        pl.when(needed)(act)


def remote(source, target, send_sem, recv_sem, device):
    return pltpu.make_async_remote_copy(
        src_ref=source,
        dst_ref=target,
        send_sem=send_sem,
        recv_sem=recv_sem,
        device_id=device,
        device_id_type=pl.DeviceIdType.MESH,
    )


def load_weights(weights, held, sems):
    copies = []
    start = 0
    for i, weight in enumerate(weights):
        cols = weight.shape[1]
        copies.append(
            pltpu.make_async_copy(weight, held.at[:, start : start + cols], sems.at[i])
        )
        start += cols
    return copies


def rows_at(index, count):
    return pl.ds(pl.multiple_of(index * count, count), count)


def gather_phase(n, ring, onward, tokens, gain, loads, s):
    rows, _ = tokens.shape
    local = n * rows
    half = rows // 2
    last = n // 2
    query_cols = s.query.shape[1]
    pair_cols = s.pairs.shape[1]
    me = lax.axis_index("tp")
    place = ring_place(me, n)
    sends = []
    halos = []

    def sender(direction, hop, chunk):
        step = -(hop - 1) if direction == 0 else hop - 1
        owner = ring_device(place + step, n)
        part = pl.ds(chunk * half, half)
        return remote(
            tokens.at[part] if hop == 1 else s.gathered.at[owner, part],
            s.gathered.at[owner, part],
            s.gather_send.at[direction, hop - 1, chunk],
            s.gather_recv.at[direction, hop - 1, chunk],
            ring[direction],
        )

    def project(sources):
        for i, (block, _) in enumerate(sources):
            values = block[...].astype(jnp.float32)
            scale = lax.rsqrt(jnp.mean(values * values, axis=1, keepdims=True) + EPS)
            s.normed[i * rows : (i + 1) * rows] = (values * scale * gain[...]).astype(jnp.bfloat16)
        count = len(sources) * rows

        def column(target, base, first):
            def write(j, carry):
                product = jnp.dot(
                    s.normed[:count],
                    s.held[:, pl.ds(pl.multiple_of(first + j * TILE, TILE), TILE)],
                    preferred_element_type=jnp.float32,
                ).astype(jnp.bfloat16)
                for i, (_, owner) in enumerate(sources):
                    at = pl.ds(pl.multiple_of(base + owner * rows, rows), rows)
                    target[at, rows_at(j, TILE)] = product[i * rows : (i + 1) * rows]
                return carry

            return write

        lax.fori_loop(0, pair_cols // TILE, column(s.pairs, 2 * local, query_cols), 0)
        for _, owner in sources:
            for back in range(2):
                source = pl.ds(pl.multiple_of(2 * local + owner * rows, rows), rows)
                target = pl.ds(pl.multiple_of((1 - back) * local + owner * rows, rows), rows)
                copy = remote(
                    s.pairs.at[source],
                    s.pairs.at[target],
                    s.halo_send.at[back, len(halos) // 2],
                    s.halo_recv.at[back, len(halos) // 2],
                    onward[back],
                )
                needed = (owner + 1) * rows > 2 * local - WINDOW if back else None
                halos.append((copy, needed))
                when(needed, copy.start)
        lax.fori_loop(0, query_cols // TILE, column(s.query, 0, 0), 0)

    for position in range(2):
        for direction in range(2):
            order = chunks_of(direction, 1, last)
            if position < len(order):
                sends.append(sender(direction, 1, order[position]))
                sends[-1].start()
    for copy in loads:
        copy.wait()
    gain[...] = s.gain_flat[...].reshape(gain.shape)
    project([(tokens, me)])
    for hop in range(1, last + 1):
        for position in range(2):
            for direction in range(2):
                order = chunks_of(direction, hop, last)
                if position < len(order):
                    chunk = order[position]
                    sender(direction, hop, chunk).wait_recv()
                    if hop < last and chunk in chunks_of(direction, hop + 1, last):
                        sends.append(sender(direction, hop + 1, chunk))
                        sends[-1].start()
        owners = [ring_device(place - hop, n)]
        if hop < last:
            owners.append(ring_device(place + hop, n))
        project([(s.gathered.at[owner], owner) for owner in owners])
    for copy, needed in halos:
        when(needed, copy.wait_recv)
    return [(copy, None) for copy in sends] + halos


def dot(lhs, rhs, left, right):
    return lax.dot_general(
        lhs, rhs, (((left,), (right,)), ((), ())), preferred_element_type=jnp.float32
    )


def attention_phase(backward, output_grad, s, meanwhile):
    local, query_cols = s.query.shape
    key_cols = s.pairs.shape[1] // 2
    kv_heads = key_cols // HEAD_SIZE
    groups = query_cols // key_cols
    reach = WINDOW - local
    span = WINDOW + QUERY_ROWS
    start = 2 * local - WINDOW
    anchor = lax.axis_index("seq") * local
    shape = (QUERY_ROWS, groups * QUERY_ROWS)
    s.gap[...] = lax.broadcasted_iota(jnp.int32, shape, 0) - (
        lax.broadcasted_iota(jnp.int32, shape, 1) % QUERY_ROWS
    )
    s.sums[...] = jnp.zeros_like(s.sums)
    sends = []

    count = local // QUERY_ROWS
    late = (count - 1) * QUERY_ROWS

    def halo(head, piece, rows):
        part = pl.ds(pl.multiple_of(piece * QUERY_ROWS, QUERY_ROWS), rows)
        return remote(
            s.leaving.at[head, part],
            s.arriving.at[head, part],
            s.back_send.at[head, piece],
            s.back_recv.at[head, piece],
            backward,
        )

    def send_back(head, piece, rows):
        part = pl.ds(pl.multiple_of(piece * QUERY_ROWS, QUERY_ROWS), rows)
        s.leaving[head, part] = s.sums[head, part].astype(jnp.bfloat16)
        halo(head, piece, rows).start()

    def lanes_of(head):
        return [
            slice((head * groups + g) * HEAD_SIZE, (head * groups + g + 1) * HEAD_SIZE)
            for g in range(groups)
        ]

    def rows_of(ref, head, i):
        own = slice(i * QUERY_ROWS, (i + 1) * QUERY_ROWS)
        return jnp.concatenate([ref[own, lanes] for lanes in lanes_of(head)], axis=0)

    def seen_by(head, i, tile, base):
        rows = slice(start + i * QUERY_ROWS + tile, start + i * QUERY_ROWS + tile + KEY_TILE)
        return s.pairs[rows, base + head * HEAD_SIZE : base + (head + 1) * HEAD_SIZE]

    def scores(head, i, slot):
        query = rows_of(s.query, head, i)
        grad = rows_of(output_grad, head, i)
        first = WINDOW - anchor - i * QUERY_ROWS
        total = jnp.zeros((8, shape[1]), jnp.float32)
        along = jnp.zeros((8, shape[1]), jnp.float32)
        for tile in range(0, span, KEY_TILE):
            bent_tile = jnp.tanh(dot(seen_by(head, i, tile, 0), query, 1, 1) * (SCALE / CAP))
            d_tile = dot(seen_by(head, i, tile, key_cols), grad, 1, 1)
            for part in range(0, KEY_TILE, QUERY_ROWS):
                row = tile + part
                bent = bent_tile[part : part + QUERY_ROWS]
                d_probs = d_tile[part : part + QUERY_ROWS]
                expo = jnp.exp2(bent * (CAP * LOG2E))
                if row == 0:
                    expo = jnp.where(s.gap[...] > jnp.where(first > 0, QUERY_ROWS, 0), expo, 0.0)
                elif row < WINDOW:
                    expo = expo * jnp.where(first > row, 0.0, 1.0)
                else:
                    expo = jnp.where(s.gap[...] <= 0, expo, 0.0)
                total += jnp.sum(expo.reshape(-1, 8, shape[1]), axis=0)
                along += jnp.sum((expo * d_probs).reshape(-1, 8, shape[1]), axis=0)
                at = slice(row, row + QUERY_ROWS)
                s.expo[slot, at] = expo.astype(jnp.bfloat16)
                s.slope[slot, at] = expo * (1.0 - bent * bent)
                s.d_probs[slot, at] = d_probs
        inverse = 1.0 / jnp.sum(total, axis=0, keepdims=True)
        delta = jnp.sum(along, axis=0, keepdims=True) * inverse
        column = jnp.transpose(jnp.broadcast_to(inverse, shape))
        return inverse, delta, column

    def gradients(head, i, slot, inverse, delta, column):
        query = (rows_of(s.query, head, i).astype(jnp.float32) * (column * SCALE)).astype(jnp.bfloat16)
        grad = (rows_of(output_grad, head, i).astype(jnp.float32) * column).astype(jnp.bfloat16)
        grad_query = jnp.zeros((shape[1], HEAD_SIZE), jnp.float32)
        for tile in range(0, span, KEY_TILE):
            rows = slice(tile, tile + KEY_TILE)
            d_raw = (s.slope[slot, rows] * (s.d_probs[slot, rows] - delta)).astype(jnp.bfloat16)
            at = slice(i * QUERY_ROWS + tile, i * QUERY_ROWS + tile + KEY_TILE)
            s.sums[head, at, :HEAD_SIZE] += dot(d_raw, query, 1, 0)
            s.sums[head, at, HEAD_SIZE:] += dot(s.expo[slot, rows], grad, 1, 0)
            grad_query += dot(d_raw, seen_by(head, i, tile, 0), 0, 0)
        grad_query = (grad_query * (column * SCALE)).astype(jnp.bfloat16)
        for g, lanes in enumerate(lanes_of(head)):
            s.grads[i * QUERY_ROWS : (i + 1) * QUERY_ROWS, lanes] = grad_query[
                g * QUERY_ROWS : (g + 1) * QUERY_ROWS
            ]

    pieces = [(piece, QUERY_ROWS) for piece in range(count - 1)] + [(count - 1, WINDOW - late)]
    steps = [(head, i) for head in range(kv_heads) for i in range(count)]
    ready = scores(*steps[0], 0)
    for k, (head, i) in enumerate(steps):
        now = ready
        if k + 1 < len(steps):
            ready = scores(*steps[k + 1], (k + 1) % 2)
        gradients(head, i, k % 2, *now)
        if i + 1 == count:
            halo(head, 0, QUERY_ROWS).wait_recv()
            s.sums[head, local:WINDOW] += s.arriving[head, :reach].astype(jnp.float32)
        send_back(head, *pieces[i])
        sends.append((halo(head, *pieces[i]), None))
    meanwhile()
    for head in range(kv_heads):
        for piece in pieces[1:]:
            halo(head, *piece).wait_recv()
        s.sums[head, WINDOW:] += s.arriving[head, reach:].astype(jnp.float32)
        for side in range(2):
            lanes = slice(side * HEAD_SIZE, (side + 1) * HEAD_SIZE)
            column = query_cols + side * key_cols + head * HEAD_SIZE
            s.grads[:, column : column + HEAD_SIZE] = s.sums[head, WINDOW:, lanes].astype(
                jnp.bfloat16
            )
    return sends


def first_owners(n):
    place = ring_place(lax.axis_index("tp"), n)
    steps = (n // 2, n // 2 - 1, 1 - n // 2)
    return [ring_device(place + step, n) for step in steps]


def later_owners(n):
    place = ring_place(lax.axis_index("tp"), n)
    steps = [step * hop for hop in range(n // 2 - 2, 0, -1) for step in (1, -1)]
    return [ring_device(place + step, n) for step in steps + [0]]


def pick(target, source, owners, rows, lanes):
    for i, owner in enumerate(owners):
        target[i * rows : (i + 1) * rows, lanes] = source[rows_at(owner, rows), lanes]


def products(total, picked, s, lanes, piece, add):
    count, width = total.shape[1:]
    for j in range(0, width, TILE):
        at = pl.ds(pl.multiple_of(piece * width + j, TILE), TILE)
        product = dot(picked[:count, lanes], s.held[at, lanes], 1, 1)
        if add:
            product += total[piece, :, j : j + TILE]
        total[piece, :, j : j + TILE] = product


def first_query_sums(n, rows, s):
    lanes = slice(0, s.query.shape[1])
    pick(s.picked_first, s.grads, first_owners(n), rows, lanes)

    def piece_sums(piece, carry):
        products(s.first, s.picked_first, s, lanes, piece, False)
        return carry

    lax.fori_loop(0, PIECES, piece_sums, 0)


def scatter_phase(n, ring, tokens, gain, out, s):
    rows, width = tokens.shape
    last = n // 2
    half = PIECES // 2
    size = width // PIECES
    cols = s.grads.shape[1]
    query_cols = s.query.shape[1]
    far = [list(range(half)), list(range(half, PIECES))]
    orders = [far[1] + far[0], far[0] + far[1]]

    def sender(direction, hop, piece):
        return remote(
            s.outgoing.at[direction, hop - 1, piece],
            s.incoming.at[direction, hop - 1, piece],
            s.scatter_send.at[direction, hop - 1, piece],
            s.scatter_recv.at[direction, hop - 1, piece],
            ring[direction],
        )

    def give(direction, hop, piece, value):
        s.outgoing[direction, hop - 1, piece] = value.astype(jnp.bfloat16)
        sender(direction, hop, piece).start()

    def take(direction, hop, piece):
        sender(direction, hop, piece).wait_recv()
        return s.incoming[direction, hop - 1, piece].astype(jnp.float32)

    lanes = slice(query_cols, cols)
    pick(s.picked_first, s.grads, first_owners(n), rows, lanes)

    def first_pair(k, carry):
        for direction in range(2):
            piece = direction * half + k
            products(s.first, s.picked_first, s, lanes, piece, True)
            other = 1 - direction
            block = (1 + other) * rows
            give(direction, last, piece, s.first[piece, :rows])
            give(other, last - 1, piece, s.first[piece, block : block + rows])
        return carry

    lax.fori_loop(0, half, first_pair, 0)
    owners = later_owners(n)
    pick(s.picked_later, s.grads, owners, rows, slice(0, cols))

    def later_sums(piece, carry):
        products(s.later, s.picked_later, s, slice(0, cols), piece, False)
        return carry

    lax.fori_loop(0, PIECES, later_sums, 0)
    values = tokens[...].astype(jnp.float32)
    scale = lax.rsqrt(jnp.mean(values * values, axis=1, keepdims=True) + EPS)
    s.unit[...] = values * scale

    for k in range(half):
        for direction in range(2):
            piece = far[direction][k]
            block = (1 + direction) * rows
            value = s.first[piece, block : block + rows]
            give(direction, last - 1, piece, value + take(direction, last, piece))
    for hop in range(last - 2, 0, -1):
        for k in range(PIECES):
            for direction in range(2):
                piece = orders[direction][k]
                block = (2 * (last - 2 - hop) + direction) * rows
                value = s.later[piece, block : block + rows]
                give(direction, hop, piece, value + take(direction, hop + 1, piece))
    along = jnp.zeros((rows, HEAD_SIZE), jnp.float32)
    block = 2 * (last - 2) * rows
    done = [set(), set()]
    for k in range(PIECES):
        for direction in range(2):
            done[direction].add(orders[direction][k])
        for piece in sorted(done[0] & done[1]):
            for direction in range(2):
                done[direction].remove(piece)
            at = slice(piece * size, (piece + 1) * size)
            value = s.later[piece, block : block + rows]
            value = value + take(0, 1, piece) + take(1, 1, piece)
            upper = value * gain[:, at]
            s.upper[:, at] = upper
            product = upper * s.unit[:, at]
            for j in range(0, size, HEAD_SIZE):
                along += product[:, j : j + HEAD_SIZE]
    mean = jnp.sum(along, axis=1, keepdims=True) * (1.0 / width)
    for piece in range(PIECES):
        at = slice(piece * size, (piece + 1) * size)
        out[:, at] = (scale * (s.upper[:, at] - s.unit[:, at] * mean)).astype(jnp.bfloat16)
    return [
        sender(direction, hop, piece)
        for hop in range(last, 0, -1)
        for direction in range(2)
        for piece in (far[direction] if hop == last else orders[direction])
    ]


def kernel(names, n, seqs, tokens_ref, gain_ref, grad_ref, wq, wk, wv, out, *scratch):
    s = types.SimpleNamespace(**dict(zip(names, scratch)))
    place = ring_place(lax.axis_index("tp"), n)
    block = lax.axis_index("seq")
    ring = [{"tp": ring_device(place + step, n)} for step in (1, -1)]
    onward = [{"seq": (block + step) % seqs} for step in (1, 2)]
    backward = [{"seq": (block + seqs - step) % seqs} for step in (1, 2)]
    greet(ring + onward + backward)
    tokens = s.tokens
    load = pltpu.make_async_copy(tokens_ref, tokens, s.load_sems.at[3])
    loads = load_weights((wq, wk, wv), s.held, s.load_sems)
    loads.append(pltpu.make_async_copy(gain_ref, s.gain_flat, s.load_sems.at[4]))
    loads.append(pltpu.make_async_copy(grad_ref, s.output_grad, s.load_sems.at[5]))
    for copy in [load] + loads:
        copy.start()
    load.wait()
    hear(ring + onward + backward)
    sends = gather_phase(n, ring, onward, tokens, s.gain, loads, s)
    meanwhile = functools.partial(first_query_sums, n, tokens.shape[0], s)
    sends += attention_phase(backward[0], s.output_grad, s, meanwhile)
    sends += [(copy, None) for copy in scatter_phase(n, ring, tokens, s.gain, out, s)]
    for copy, needed in sends:
        when(needed, copy.wait_send)


def on_device(tokens, norm_gain, query_weight, key_matrix, value_matrix, output_grad):
    n = lax.axis_size("tp")
    rows, width = tokens.shape
    local, query_cols = output_grad.shape
    key_cols = key_matrix.shape[1]
    cols = query_cols + 2 * key_cols
    kv_heads = key_cols // HEAD_SIZE
    groups = query_cols // key_cols
    low, full = jnp.bfloat16, jnp.float32
    hops = pltpu.SemaphoreType.DMA((2, n // 2, 2))
    pieces = pltpu.SemaphoreType.DMA((2, n // 2, PIECES))
    blocks = pltpu.SemaphoreType.DMA((2, n))
    heads = pltpu.SemaphoreType.DMA((kv_heads, local // QUERY_ROWS))
    scratch = dict(
        tokens=pltpu.VMEM((rows, width), low),
        output_grad=pltpu.VMEM((local, query_cols), low),
        gain_flat=pltpu.VMEM((width,), full),
        gain=pltpu.VMEM((1, width), full),
        gathered=pltpu.VMEM((n, rows, width), low),
        held=pltpu.VMEM((width, cols), low),
        normed=pltpu.VMEM((2 * rows, width), low),
        query=pltpu.VMEM((local, query_cols), low),
        pairs=pltpu.VMEM((3 * local, 2 * key_cols), low),
        gap=pltpu.VMEM((QUERY_ROWS, groups * QUERY_ROWS), jnp.int32),
        expo=pltpu.VMEM((2, WINDOW + QUERY_ROWS, groups * QUERY_ROWS), low),
        slope=pltpu.VMEM((2, WINDOW + QUERY_ROWS, groups * QUERY_ROWS), full),
        d_probs=pltpu.VMEM((2, WINDOW + QUERY_ROWS, groups * QUERY_ROWS), full),
        sums=pltpu.VMEM((kv_heads, WINDOW + local, 2 * HEAD_SIZE), full),
        leaving=pltpu.VMEM((kv_heads, WINDOW, 2 * HEAD_SIZE), low),
        arriving=pltpu.VMEM((kv_heads, WINDOW, 2 * HEAD_SIZE), low),
        grads=pltpu.VMEM((local, cols), low),
        outgoing=pltpu.VMEM((2, n // 2, PIECES, rows, width // PIECES), low),
        incoming=pltpu.VMEM((2, n // 2, PIECES, rows, width // PIECES), low),
        picked_first=pltpu.VMEM((3 * rows, cols), low),
        picked_later=pltpu.VMEM(((n - 3) * rows, cols), low),
        first=pltpu.VMEM((PIECES, 3 * rows, width // PIECES), full),
        later=pltpu.VMEM((PIECES, (n - 3) * rows, width // PIECES), full),
        unit=pltpu.VMEM((rows, width), full),
        upper=pltpu.VMEM((rows, width), full),
        gather_send=hops,
        gather_recv=hops,
        halo_send=blocks,
        halo_recv=blocks,
        back_send=heads,
        back_recv=heads,
        scatter_send=pieces,
        scatter_recv=pieces,
        load_sems=pltpu.SemaphoreType.DMA((6,)),
    )
    vmem = pl.BlockSpec(memory_space=pltpu.VMEM)
    hbm = pl.BlockSpec(memory_space=pl.ANY)
    return pl.pallas_call(
        functools.partial(kernel, tuple(scratch), n, lax.axis_size("seq")),
        out_shape=pltpu.VMEM((rows, width), low),
        in_specs=[hbm] * 6,
        out_specs=vmem,
        scratch_shapes=list(scratch.values()),
        compiler_params=pltpu.CompilerParams(
            collective_id=0, has_side_effects=True, vmem_limit_bytes=VMEM_BYTES
        ),
        name="attention_backward",
    )(tokens, norm_gain, output_grad, query_weight, key_matrix, value_matrix)


def solution(mesh):
    return jax.shard_map(
        on_device,
        mesh=mesh,
        in_specs=(
            P(("seq", "tp"), None),
            P(),
            P(None, "tp"),
            P(None, "tp"),
            P(None, "tp"),
            P("seq", "tp"),
        ),
        out_specs=P(("seq", "tp"), None),
        check_vma=False,
    )
```

```python
import functools
import types

import jax
import jax.numpy as jnp
from jax import lax
from jax.experimental import pallas as pl
from jax.experimental.pallas import tpu as pltpu
from jax.sharding import PartitionSpec as P

HEAD_SIZE = 128
WINDOW = 640


SCALE = 1.0 / 12.0
CAP = 50.0
EPS = 1e-06
VMEM_BYTES = 60 * 1024 * 1024
QUERY_ROWS = 128
KEY_TILE = 256
PIECES = 6
LOG2E = 1.4426950408889634
TILE = 256


def ring_place(index, n):
    odd = index % 2
    return (1 - odd) * (index // 2) + odd * (n - 1 - index // 2)


def ring_device(place, n):
    place = (place + n) % n
    late = place // (n // 2)
    return (1 - late) * 2 * place + late * (2 * (n - 1 - place) + 1)


def chunks_of(direction, hop, last):
    return (direction, 1 - direction) if hop < last else (direction,)


def greet(neighbours):
    barrier = pltpu.get_barrier_semaphore()
    for neighbour in neighbours:
        pl.semaphore_signal(
            barrier, inc=1, device_id=neighbour, device_id_type=pl.DeviceIdType.MESH
        )


def hear(neighbours):
    pl.semaphore_wait(pltpu.get_barrier_semaphore(), len(neighbours))


def when(needed, act):
    if needed is None:
        act()
    else:
        pl.when(needed)(act)


def remote(source, target, send_sem, recv_sem, device):
    return pltpu.make_async_remote_copy(
        src_ref=source,
        dst_ref=target,
        send_sem=send_sem,
        recv_sem=recv_sem,
        device_id=device,
        device_id_type=pl.DeviceIdType.MESH,
    )


def load_weights(weights, held, sems):
    copies = []
    start = 0
    for i, weight in enumerate(weights):
        cols = weight.shape[1]
        copies.append(
            pltpu.make_async_copy(weight, held.at[:, start : start + cols], sems.at[i])
        )
        start += cols
    return copies


def rows_at(index, count):
    return pl.ds(pl.multiple_of(index * count, count), count)


def gather_phase(n, ring, onward, tokens, gain, loads, s):
    rows, _ = tokens.shape
    local = n * rows
    half = rows // 2
    last = n // 2
    query_cols = s.query.shape[1]
    pair_cols = s.pairs.shape[1]
    me = lax.axis_index("tp")
    place = ring_place(me, n)
    sends = []
    halos = []

    def sender(direction, hop, chunk):
        step = -(hop - 1) if direction == 0 else hop - 1
        owner = ring_device(place + step, n)
        part = pl.ds(chunk * half, half)
        return remote(
            tokens.at[part] if hop == 1 else s.gathered.at[owner, part],
            s.gathered.at[owner, part],
            s.gather_send.at[direction, hop - 1, chunk],
            s.gather_recv.at[direction, hop - 1, chunk],
            ring[direction],
        )

    def project(sources):
        for i, (block, _) in enumerate(sources):
            values = block[...].astype(jnp.float32)
            scale = lax.rsqrt(jnp.mean(values * values, axis=1, keepdims=True) + EPS)
            s.normed[i * rows : (i + 1) * rows] = (values * scale * gain[...]).astype(jnp.bfloat16)
        count = len(sources) * rows

        def column(target, base, first):
            def write(j, carry):
                product = jnp.dot(
                    s.normed[:count],
                    s.held[:, pl.ds(pl.multiple_of(first + j * TILE, TILE), TILE)],
                    preferred_element_type=jnp.float32,
                ).astype(jnp.bfloat16)
                for i, (_, owner) in enumerate(sources):
                    at = pl.ds(pl.multiple_of(base + owner * rows, rows), rows)
                    target[at, rows_at(j, TILE)] = product[i * rows : (i + 1) * rows]
                return carry

            return write

        lax.fori_loop(0, pair_cols // TILE, column(s.pairs, 2 * local, query_cols), 0)
        for _, owner in sources:
            for back in range(2):
                source = pl.ds(pl.multiple_of(2 * local + owner * rows, rows), rows)
                target = pl.ds(pl.multiple_of((1 - back) * local + owner * rows, rows), rows)
                copy = remote(
                    s.pairs.at[source],
                    s.pairs.at[target],
                    s.halo_send.at[back, len(halos) // 2],
                    s.halo_recv.at[back, len(halos) // 2],
                    onward[back],
                )
                needed = (owner + 1) * rows > 2 * local - WINDOW if back else None
                halos.append((copy, needed))
                when(needed, copy.start)
        lax.fori_loop(0, query_cols // TILE, column(s.query, 0, 0), 0)

    for position in range(2):
        for direction in range(2):
            order = chunks_of(direction, 1, last)
            if position < len(order):
                sends.append(sender(direction, 1, order[position]))
                sends[-1].start()
    for copy in loads:
        copy.wait()
    gain[...] = s.gain_flat[...].reshape(gain.shape)
    project([(tokens, me)])
    prepare_attention(s)
    for hop in range(1, last + 1):
        for position in range(2):
            for direction in range(2):
                order = chunks_of(direction, hop, last)
                if position < len(order):
                    chunk = order[position]
                    sender(direction, hop, chunk).wait_recv()
                    if hop < last and chunk in chunks_of(direction, hop + 1, last):
                        sends.append(sender(direction, hop + 1, chunk))
                        sends[-1].start()
        owners = [ring_device(place - hop, n)]
        if hop < last:
            owners.append(ring_device(place + hop, n))
        project([(s.gathered.at[owner], owner) for owner in owners])
    for copy, needed in halos:
        when(needed, copy.wait_recv)
    return [(copy, None) for copy in sends] + halos


def dot(lhs, rhs, left, right):
    return lax.dot_general(
        lhs, rhs, (((left,), (right,)), ((), ())), preferred_element_type=jnp.float32
    )


def prepare_attention(s):
    shape = s.gap.shape
    s.gap[...] = lax.broadcasted_iota(jnp.int32, shape, 0) - (
        lax.broadcasted_iota(jnp.int32, shape, 1) % QUERY_ROWS
    )
    s.sums[...] = jnp.zeros_like(s.sums)


def attention_phase(n, rows, backward, output_grad, s):
    local, query_cols = s.query.shape
    key_cols = s.pairs.shape[1] // 2
    kv_heads = key_cols // HEAD_SIZE
    groups = query_cols // key_cols
    reach = WINDOW - local
    span = WINDOW + QUERY_ROWS
    start = 2 * local - WINDOW
    anchor = lax.axis_index("seq") * local
    shape = s.gap.shape
    sends = []

    count = local // QUERY_ROWS
    late = (count - 1) * QUERY_ROWS

    def halo(head, piece, rows):
        part = pl.ds(pl.multiple_of(piece * QUERY_ROWS, QUERY_ROWS), rows)
        return remote(
            s.leaving.at[head, part],
            s.arriving.at[head, part],
            s.back_send.at[head, piece],
            s.back_recv.at[head, piece],
            backward,
        )

    def send_back(head, piece, rows):
        part = pl.ds(pl.multiple_of(piece * QUERY_ROWS, QUERY_ROWS), rows)
        s.leaving[head, part] = s.sums[head, part].astype(jnp.bfloat16)
        halo(head, piece, rows).start()

    def lanes_of(head):
        return [
            slice((head * groups + g) * HEAD_SIZE, (head * groups + g + 1) * HEAD_SIZE)
            for g in range(groups)
        ]

    def rows_of(ref, head, i):
        own = slice(i * QUERY_ROWS, (i + 1) * QUERY_ROWS)
        return jnp.concatenate([ref[own, lanes] for lanes in lanes_of(head)], axis=0)

    def seen_by(head, i, tile, base):
        rows = slice(start + i * QUERY_ROWS + tile, start + i * QUERY_ROWS + tile + KEY_TILE)
        return s.pairs[rows, base + head * HEAD_SIZE : base + (head + 1) * HEAD_SIZE]

    def scores(head, i, slot):
        query = rows_of(s.query, head, i)
        grad = rows_of(output_grad, head, i)
        first = WINDOW - anchor - i * QUERY_ROWS
        total = jnp.zeros((8, shape[1]), jnp.float32)
        along = jnp.zeros((8, shape[1]), jnp.float32)
        for tile in range(0, span, KEY_TILE):
            bent_tile = jnp.tanh(dot(seen_by(head, i, tile, 0), query, 1, 1) * (SCALE / CAP))
            d_tile = dot(seen_by(head, i, tile, key_cols), grad, 1, 1)
            for part in range(0, KEY_TILE, QUERY_ROWS):
                row = tile + part
                bent = bent_tile[part : part + QUERY_ROWS]
                d_probs = d_tile[part : part + QUERY_ROWS]
                expo = jnp.exp2(bent * (CAP * LOG2E))
                if row == 0:
                    expo = jnp.where(s.gap[...] > jnp.where(first > 0, QUERY_ROWS, 0), expo, 0.0)
                elif row < WINDOW:
                    expo = expo * jnp.where(first > row, 0.0, 1.0)
                else:
                    expo = jnp.where(s.gap[...] <= 0, expo, 0.0)
                total += jnp.sum(expo.reshape(-1, 8, shape[1]), axis=0)
                along += jnp.sum((expo * d_probs).reshape(-1, 8, shape[1]), axis=0)
                at = slice(row, row + QUERY_ROWS)
                s.expo[slot, at] = expo.astype(jnp.bfloat16)
                s.slope[slot, at] = expo * (1.0 - bent * bent)
                s.d_probs[slot, at] = d_probs
        inverse = 1.0 / jnp.sum(total, axis=0, keepdims=True)
        delta = jnp.sum(along, axis=0, keepdims=True) * inverse
        column = jnp.transpose(jnp.broadcast_to(inverse, shape))
        return inverse, delta, column

    def gradients(head, i, slot, inverse, delta, column):
        query = (rows_of(s.query, head, i).astype(jnp.float32) * (column * SCALE)).astype(jnp.bfloat16)
        grad = (rows_of(output_grad, head, i).astype(jnp.float32) * column).astype(jnp.bfloat16)
        grad_query = jnp.zeros((shape[1], HEAD_SIZE), jnp.float32)
        for tile in range(0, span, KEY_TILE):
            rows = slice(tile, tile + KEY_TILE)
            d_raw = (s.slope[slot, rows] * (s.d_probs[slot, rows] - delta)).astype(jnp.bfloat16)
            at = slice(i * QUERY_ROWS + tile, i * QUERY_ROWS + tile + KEY_TILE)
            s.sums[head, at, :HEAD_SIZE] += dot(d_raw, query, 1, 0)
            s.sums[head, at, HEAD_SIZE:] += dot(s.expo[slot, rows], grad, 1, 0)
            grad_query += dot(d_raw, seen_by(head, i, tile, 0), 0, 0)
        grad_query = (grad_query * (column * SCALE)).astype(jnp.bfloat16)
        for g, lanes in enumerate(lanes_of(head)):
            s.grads[i * QUERY_ROWS : (i + 1) * QUERY_ROWS, lanes] = grad_query[
                g * QUERY_ROWS : (g + 1) * QUERY_ROWS
            ]

    pieces = [(piece, QUERY_ROWS) for piece in range(count - 1)] + [(count - 1, WINDOW - late)]
    steps = [(head, i) for i in range(count) for head in range(kv_heads)]
    ready = scores(*steps[0], 0)
    for k, (head, i) in enumerate(steps):
        now = ready
        if k + 1 < len(steps):
            ready = scores(*steps[k + 1], (k + 1) % 2)
        gradients(head, i, k % 2, *now)
        if i + 1 == count:
            halo(head, 0, QUERY_ROWS).wait_recv()
            s.sums[head, local:WINDOW] += s.arriving[head, :reach].astype(jnp.float32)
        send_back(head, *pieces[i])
        sends.append((halo(head, *pieces[i]), None))
    owners = first_owners(n)
    pick(s.picked_first, s.grads, owners, slice(0, query_cols), rows)
    for head in range(kv_heads):
        for piece in pieces[1:]:
            halo(head, *piece).wait_recv()
    columns = [
        (head, side, query_cols + side * key_cols + head * HEAD_SIZE)
        for head in range(kv_heads)
        for side in range(2)
    ]
    for head, side, column in columns:
        lanes = slice(side * HEAD_SIZE, (side + 1) * HEAD_SIZE)
        for i, owner in enumerate(owners):
            own = pl.ds(pl.multiple_of(WINDOW + owner * rows, rows), rows)
            far = pl.ds(pl.multiple_of(reach + owner * rows, rows), rows)
            value = s.sums[head, own, lanes] + s.arriving[head, far, lanes].astype(jnp.float32)
            s.picked_first[i * rows : (i + 1) * rows, column : column + HEAD_SIZE] = value.astype(
                jnp.bfloat16
            )

    def rest():
        for head, side, column in columns:
            lanes = slice(side * HEAD_SIZE, (side + 1) * HEAD_SIZE)
            value = s.sums[head, WINDOW:, lanes] + s.arriving[head, reach:, lanes].astype(jnp.float32)
            s.grads[:, column : column + HEAD_SIZE] = value.astype(jnp.bfloat16)

    return sends, rest


def first_owners(n):
    place = ring_place(lax.axis_index("tp"), n)
    steps = (n // 2, n // 2 - 1, 1 - n // 2)
    return [ring_device(place + step, n) for step in steps]


def later_owners(n):
    place = ring_place(lax.axis_index("tp"), n)
    steps = [step * hop for hop in range(n // 2 - 2, 0, -1) for step in (1, -1)]
    return [ring_device(place + step, n) for step in steps + [0]]


def pick(target, source, owners, lanes, rows):
    for i, owner in enumerate(owners):
        target[i * rows : (i + 1) * rows, lanes] = source[rows_at(owner, rows), lanes]


def products(total, picked, s, piece):
    count, width = total.shape[1:]
    for j in range(0, width, TILE):
        at = pl.ds(pl.multiple_of(piece * width + j, TILE), TILE)
        total[piece, :, j : j + TILE] = dot(picked[:count], s.held[at], 1, 1)


def scatter_phase(n, ring, tokens, gain, out, rest, s):
    rows, width = tokens.shape
    last = n // 2
    half = PIECES // 2
    size = width // PIECES
    cols = s.grads.shape[1]
    far = [list(range(half)), list(range(half, PIECES))]

    def sender(direction, hop, piece):
        return remote(
            s.outgoing.at[direction, hop - 1, piece],
            s.incoming.at[direction, hop - 1, piece],
            s.scatter_send.at[direction, hop - 1, piece],
            s.scatter_recv.at[direction, hop - 1, piece],
            ring[direction],
        )

    def bundle(direction, hop, side):
        part = pl.ds(side * half, half)
        return remote(
            s.outgoing.at[direction, hop - 1, part],
            s.incoming.at[direction, hop - 1, part],
            s.scatter_send.at[direction, hop - 1, side * half],
            s.scatter_recv.at[direction, hop - 1, side * half],
            ring[direction],
        )

    def parcels(direction, hop, side):
        if hop == last or (hop == last - 1 and side != direction):
            return [sender(direction, hop, piece) for piece in far[side]]
        return [bundle(direction, hop, side)]

    def give(direction, hop, piece, value):
        s.outgoing[direction, hop - 1, piece] = value.astype(jnp.bfloat16)
        sender(direction, hop, piece).start()

    def arrive(direction, hop, side):
        for copy in parcels(direction, hop, side):
            copy.wait_recv()

    def relay(direction, hop, side, source, block):
        arrive(direction, hop + 1, side)
        for piece in far[side]:
            value = source[piece, block : block + rows]
            value += s.incoming[direction, hop, piece].astype(jnp.float32)
            s.outgoing[direction, hop - 1, piece] = value.astype(jnp.bfloat16)
        bundle(direction, hop, side).start()

    def first_pair(k, carry):
        for direction in range(2):
            piece = direction * half + k
            products(s.first, s.picked_first, s, piece)
            other = 1 - direction
            block = (1 + other) * rows
            give(direction, last, piece, s.first[piece, :rows])
            give(other, last - 1, piece, s.first[piece, block : block + rows])
        return carry

    lax.fori_loop(0, half, first_pair, 0)
    owners = later_owners(n)
    rest()
    pick(s.picked_later, s.grads, owners, slice(0, cols), rows)

    def later_sums(piece, carry):
        products(s.later, s.picked_later, s, piece)
        return carry

    lax.fori_loop(0, PIECES, later_sums, 0)
    values = tokens[...].astype(jnp.float32)
    scale = lax.rsqrt(jnp.mean(values * values, axis=1, keepdims=True) + EPS)
    s.unit[...] = values * scale

    for direction in range(2):
        relay(direction, last - 1, direction, s.first, (1 + direction) * rows)
    for hop in range(last - 2, 0, -1):
        for turn in range(2):
            for direction in range(2):
                side = direction if turn else 1 - direction
                block = (2 * (last - 2 - hop) + direction) * rows
                relay(direction, hop, side, s.later, block)
    along = jnp.zeros((rows, HEAD_SIZE), jnp.float32)
    block = 2 * (last - 2) * rows
    for direction in range(2):
        side = 1 - direction
        arrive(direction, 1, side)
        for piece in far[side]:
            s.later[piece, block : block + rows] += s.incoming[direction, 0, piece].astype(jnp.float32)
    for direction in range(2):
        arrive(direction, 1, direction)
        for piece in far[direction]:
            at = slice(piece * size, (piece + 1) * size)
            value = s.later[piece, block : block + rows]
            value += s.incoming[direction, 0, piece].astype(jnp.float32)
            upper = value * gain[:, at]
            s.upper[:, at] = upper
            product = upper * s.unit[:, at]
            for j in range(0, size, HEAD_SIZE):
                along += product[:, j : j + HEAD_SIZE]
    mean = jnp.sum(along, axis=1, keepdims=True) * (1.0 / width)
    for piece in range(PIECES):
        at = slice(piece * size, (piece + 1) * size)
        out[:, at] = (scale * (s.upper[:, at] - s.unit[:, at] * mean)).astype(jnp.bfloat16)
    return [
        copy
        for hop in range(last, 0, -1)
        for direction in range(2)
        for side in range(2)
        if hop < last or side == direction
        for copy in parcels(direction, hop, side)
    ]


def kernel(names, n, seqs, tokens_ref, gain_ref, grad_ref, wq, wk, wv, out, *scratch):
    s = types.SimpleNamespace(**dict(zip(names, scratch)))
    place = ring_place(lax.axis_index("tp"), n)
    block = lax.axis_index("seq")
    ring = [{"tp": ring_device(place + step, n)} for step in (1, -1)]
    onward = [{"seq": (block + step) % seqs} for step in (1, 2)]
    backward = [{"seq": (block + seqs - step) % seqs} for step in (1, 2)]
    greet(ring + onward + backward)
    tokens = s.tokens
    load = pltpu.make_async_copy(tokens_ref, tokens, s.load_sems.at[3])
    loads = load_weights((wq, wk, wv), s.held, s.load_sems)
    loads.append(pltpu.make_async_copy(gain_ref, s.gain_flat, s.load_sems.at[4]))
    loads.append(pltpu.make_async_copy(grad_ref, s.output_grad, s.load_sems.at[5]))
    for copy in [load] + loads:
        copy.start()
    load.wait()
    hear(ring + onward + backward)
    sends = gather_phase(n, ring, onward, tokens, s.gain, loads, s)
    halos, rest = attention_phase(n, tokens.shape[0], backward[0], s.output_grad, s)
    sends += halos
    sends += [(copy, None) for copy in scatter_phase(n, ring, tokens, s.gain, out, rest, s)]
    for copy, needed in sends:
        when(needed, copy.wait_send)


def on_device(tokens, norm_gain, query_weight, key_matrix, value_matrix, output_grad):
    n = lax.axis_size("tp")
    rows, width = tokens.shape
    local, query_cols = output_grad.shape
    key_cols = key_matrix.shape[1]
    cols = query_cols + 2 * key_cols
    kv_heads = key_cols // HEAD_SIZE
    groups = query_cols // key_cols
    low, full = jnp.bfloat16, jnp.float32
    hops = pltpu.SemaphoreType.DMA((2, n // 2, 2))
    pieces = pltpu.SemaphoreType.DMA((2, n // 2, PIECES))
    blocks = pltpu.SemaphoreType.DMA((2, n))
    heads = pltpu.SemaphoreType.DMA((kv_heads, local // QUERY_ROWS))
    scratch = dict(
        tokens=pltpu.VMEM((rows, width), low),
        output_grad=pltpu.VMEM((local, query_cols), low),
        gain_flat=pltpu.VMEM((width,), full),
        gain=pltpu.VMEM((1, width), full),
        gathered=pltpu.VMEM((n, rows, width), low),
        held=pltpu.VMEM((width, cols), low),
        normed=pltpu.VMEM((2 * rows, width), low),
        query=pltpu.VMEM((local, query_cols), low),
        pairs=pltpu.VMEM((3 * local, 2 * key_cols), low),
        gap=pltpu.VMEM((QUERY_ROWS, groups * QUERY_ROWS), jnp.int32),
        expo=pltpu.VMEM((2, WINDOW + QUERY_ROWS, groups * QUERY_ROWS), low),
        slope=pltpu.VMEM((2, WINDOW + QUERY_ROWS, groups * QUERY_ROWS), full),
        d_probs=pltpu.VMEM((2, WINDOW + QUERY_ROWS, groups * QUERY_ROWS), full),
        sums=pltpu.VMEM((kv_heads, WINDOW + local, 2 * HEAD_SIZE), full),
        leaving=pltpu.VMEM((kv_heads, WINDOW, 2 * HEAD_SIZE), low),
        arriving=pltpu.VMEM((kv_heads, WINDOW, 2 * HEAD_SIZE), low),
        grads=pltpu.VMEM((local, cols), low),
        outgoing=pltpu.VMEM((2, n // 2, PIECES, rows, width // PIECES), low),
        incoming=pltpu.VMEM((2, n // 2, PIECES, rows, width // PIECES), low),
        picked_first=pltpu.VMEM((3 * rows, cols), low),
        picked_later=pltpu.VMEM(((n - 3) * rows, cols), low),
        first=pltpu.VMEM((PIECES, 3 * rows, width // PIECES), full),
        later=pltpu.VMEM((PIECES, (n - 3) * rows, width // PIECES), full),
        unit=pltpu.VMEM((rows, width), full),
        upper=pltpu.VMEM((rows, width), full),
        gather_send=hops,
        gather_recv=hops,
        halo_send=blocks,
        halo_recv=blocks,
        back_send=heads,
        back_recv=heads,
        scatter_send=pieces,
        scatter_recv=pieces,
        load_sems=pltpu.SemaphoreType.DMA((6,)),
    )
    vmem = pl.BlockSpec(memory_space=pltpu.VMEM)
    hbm = pl.BlockSpec(memory_space=pl.ANY)
    return pl.pallas_call(
        functools.partial(kernel, tuple(scratch), n, lax.axis_size("seq")),
        out_shape=pltpu.VMEM((rows, width), low),
        in_specs=[hbm] * 6,
        out_specs=vmem,
        scratch_shapes=list(scratch.values()),
        compiler_params=pltpu.CompilerParams(
            collective_id=0, has_side_effects=True, vmem_limit_bytes=VMEM_BYTES
        ),
        name="attention_backward",
    )(tokens, norm_gain, output_grad, query_weight, key_matrix, value_matrix)


def solution(mesh):
    return jax.shard_map(
        on_device,
        mesh=mesh,
        in_specs=(
            P(("seq", "tp"), None),
            P(),
            P(None, "tp"),
            P(None, "tp"),
            P(None, "tp"),
            P("seq", "tp"),
        ),
        out_specs=P(("seq", "tp"), None),
        check_vma=False,
    )
```

```python
import functools
import types

import jax
import jax.numpy as jnp
from jax import lax
from jax.experimental import pallas as pl
from jax.experimental.pallas import tpu as pltpu
from jax.sharding import PartitionSpec as P

HEAD_SIZE = 128
WINDOW = 640


SCALE = 1.0 / 12.0
CAP = 50.0
EPS = 1e-06
VMEM_BYTES = 60 * 1024 * 1024
QUERY_ROWS = 128
KEY_TILE = 256
PIECES = 6
LOG2E = 1.4426950408889634
TILE = 256


def ring_place(index, n):
    odd = index % 2
    return (1 - odd) * (index // 2) + odd * (n - 1 - index // 2)


def ring_device(place, n):
    place = (place + n) % n
    late = place // (n // 2)
    return (1 - late) * 2 * place + late * (2 * (n - 1 - place) + 1)


def chunks_of(direction, hop, last):
    return (direction, 1 - direction) if hop < last else (direction,)


def greet(neighbours):
    barrier = pltpu.get_barrier_semaphore()
    for neighbour in neighbours:
        pl.semaphore_signal(
            barrier, inc=1, device_id=neighbour, device_id_type=pl.DeviceIdType.MESH
        )


def hear(neighbours):
    pl.semaphore_wait(pltpu.get_barrier_semaphore(), len(neighbours))


def when(needed, act):
    if needed is None:
        act()
    else:
        pl.when(needed)(act)


def remote(source, target, send_sem, recv_sem, device):
    return pltpu.make_async_remote_copy(
        src_ref=source,
        dst_ref=target,
        send_sem=send_sem,
        recv_sem=recv_sem,
        device_id=device,
        device_id_type=pl.DeviceIdType.MESH,
    )


def load_weights(weights, held, sems):
    copies = []
    start = 0
    for i, weight in enumerate(weights):
        cols = weight.shape[1]
        copies.append(
            pltpu.make_async_copy(weight, held.at[:, start : start + cols], sems.at[i])
        )
        start += cols
    return copies


def rows_at(index, count):
    return pl.ds(pl.multiple_of(index * count, count), count)


def gather_phase(n, ring, onward, tokens, gain, loads, s):
    rows, _ = tokens.shape
    local = n * rows
    half = rows // 2
    quarter = half // 2
    last = n // 2
    query_cols = s.query.shape[1]
    pair_cols = s.pairs.shape[1]
    me = lax.axis_index("tp")
    place = ring_place(me, n)
    sends = []
    halos = []

    def sender(direction, hop, chunk):
        step = -(hop - 1) if direction == 0 else hop - 1
        owner = ring_device(place + step, n)
        part = pl.ds(chunk * half, half)
        return remote(
            tokens.at[part] if hop == 1 else s.gathered.at[owner, part],
            s.gathered.at[owner, part],
            s.gather_send.at[direction, hop - 1, chunk],
            s.gather_recv.at[direction, hop - 1, chunk],
            ring[direction],
        )

    def last_sender(direction, stage):
        owner = ring_device(place + (1 - last if direction == 0 else last - 1), n)
        part = pl.ds(direction * half + stage * quarter, quarter)
        return remote(
            s.gathered.at[owner, part],
            s.gathered.at[owner, part],
            s.gather_send.at[direction, last - 1, stage],
            s.gather_recv.at[direction, last - 1, stage],
            ring[direction],
        )

    def normalize(pieces, at):
        for block, _, size in pieces:
            values = block[...].astype(jnp.float32)
            scale = lax.rsqrt(jnp.mean(values * values, axis=1, keepdims=True) + EPS)
            s.normed[at : at + size] = (values * scale * gain[...]).astype(jnp.bfloat16)
            at += size

    def columns(pieces, at, tiles, target, base, first):
        count = sum(size for _, _, size in pieces)

        def write(j, carry):
            product = jnp.dot(
                s.normed[at : at + count],
                s.held[:, pl.ds(pl.multiple_of(first + j * TILE, TILE), TILE)],
                preferred_element_type=jnp.float32,
            ).astype(jnp.bfloat16)
            done = 0
            for _, row, size in pieces:
                to = pl.ds(pl.multiple_of(base + row, size), size)
                target[to, rows_at(j, TILE)] = product[done : done + size]
                done += size
            return carry

        lax.fori_loop(0, tiles, write, 0)

    def pairs(pieces, at):
        columns(pieces, at, pair_cols // TILE, s.pairs, 2 * local, query_cols)
        for _, row, size in pieces:
            for back in range(2):
                copy = remote(
                    s.pairs.at[pl.ds(pl.multiple_of(2 * local + row, size), size)],
                    s.pairs.at[pl.ds(pl.multiple_of((1 - back) * local + row, size), size)],
                    s.halo_send.at[back, len(halos) // 2],
                    s.halo_recv.at[back, len(halos) // 2],
                    onward[back],
                )
                needed = row + size > 2 * local - WINDOW if back else None
                halos.append((copy, needed))
                when(needed, copy.start)

    def queries(pieces, at):
        columns(pieces, at, query_cols // TILE, s.query, 0, 0)

    def project(sources):
        pieces = [(block, owner * rows, rows) for block, owner in sources]
        normalize(pieces, 0)
        pairs(pieces, 0)
        queries(pieces, 0)

    for position in range(2):
        for direction in range(2):
            order = chunks_of(direction, 1, last)
            if position < len(order):
                sends.append(sender(direction, 1, order[position]))
                sends[-1].start()
    for copy in loads:
        copy.wait()
    gain[...] = s.gain_flat[...].reshape(gain.shape)
    project([(tokens, me)])
    prepare_attention(s)
    for hop in range(1, last):
        for position in range(2):
            for direction in range(2):
                chunk = chunks_of(direction, hop, last)[position]
                sender(direction, hop, chunk).wait_recv()
                if hop + 1 < last:
                    sends.append(sender(direction, hop + 1, chunk))
                    sends[-1].start()
                elif chunk == direction:
                    for stage in range(2):
                        sends.append(last_sender(direction, stage))
                        sends[-1].start()
        owners = [ring_device(place - hop, n), ring_device(place + hop, n)]
        project([(s.gathered.at[owner], owner) for owner in owners])
    owner = ring_device(place + last, n)
    pieces = []
    for stage in range(2):
        for direction in range(2):
            last_sender(direction, stage).wait_recv()
            first = direction * half + stage * quarter
            block = s.gathered.at[owner, first : first + quarter]
            pieces.append((block, owner * rows + first, quarter))
        normalize(pieces[2 * stage :], stage * half)
        pairs(pieces[2 * stage :], stage * half)
    queries(pieces, 0)
    for copy, needed in halos:
        when(needed, copy.wait_recv)
    return [(copy, None) for copy in sends] + halos


def dot(lhs, rhs, left, right):
    return lax.dot_general(
        lhs, rhs, (((left,), (right,)), ((), ())), preferred_element_type=jnp.float32
    )


def prepare_attention(s):
    shape = s.gap.shape
    s.gap[...] = lax.broadcasted_iota(jnp.int32, shape, 0) - (
        lax.broadcasted_iota(jnp.int32, shape, 1) % QUERY_ROWS
    )
    s.sums[...] = jnp.zeros_like(s.sums)


def attention_phase(n, rows, backward, output_grad, s):
    local, query_cols = s.query.shape
    key_cols = s.pairs.shape[1] // 2
    kv_heads = key_cols // HEAD_SIZE
    groups = query_cols // key_cols
    reach = WINDOW - local
    span = WINDOW + QUERY_ROWS
    start = 2 * local - WINDOW
    anchor = lax.axis_index("seq") * local
    shape = s.gap.shape
    sends = []

    count = local // QUERY_ROWS
    late = (count - 1) * QUERY_ROWS

    def halo(head, piece, rows):
        part = pl.ds(pl.multiple_of(piece * QUERY_ROWS, QUERY_ROWS), rows)
        return remote(
            s.leaving.at[head, part],
            s.arriving.at[head, part],
            s.back_send.at[head, piece],
            s.back_recv.at[head, piece],
            backward,
        )

    def send_back(head, piece, rows):
        part = pl.ds(pl.multiple_of(piece * QUERY_ROWS, QUERY_ROWS), rows)
        s.leaving[head, part] = s.sums[head, part].astype(jnp.bfloat16)
        halo(head, piece, rows).start()

    def lanes_of(head):
        return [
            slice((head * groups + g) * HEAD_SIZE, (head * groups + g + 1) * HEAD_SIZE)
            for g in range(groups)
        ]

    def rows_of(ref, head, i):
        own = slice(i * QUERY_ROWS, (i + 1) * QUERY_ROWS)
        return jnp.concatenate([ref[own, lanes] for lanes in lanes_of(head)], axis=0)

    def seen_by(head, i, tile, base):
        rows = slice(start + i * QUERY_ROWS + tile, start + i * QUERY_ROWS + tile + KEY_TILE)
        return s.pairs[rows, base + head * HEAD_SIZE : base + (head + 1) * HEAD_SIZE]

    def scores(head, i, slot):
        query = rows_of(s.query, head, i)
        grad = rows_of(output_grad, head, i)
        first = WINDOW - anchor - i * QUERY_ROWS
        total = jnp.zeros((8, shape[1]), jnp.float32)
        along = jnp.zeros((8, shape[1]), jnp.float32)
        for tile in range(0, span, KEY_TILE):
            bent_tile = jnp.tanh(dot(seen_by(head, i, tile, 0), query, 1, 1) * (SCALE / CAP))
            d_tile = dot(seen_by(head, i, tile, key_cols), grad, 1, 1)
            for part in range(0, KEY_TILE, QUERY_ROWS):
                row = tile + part
                bent = bent_tile[part : part + QUERY_ROWS]
                d_probs = d_tile[part : part + QUERY_ROWS]
                expo = jnp.exp2(bent * (CAP * LOG2E))
                if row == 0:
                    expo = jnp.where(s.gap[...] > jnp.where(first > 0, QUERY_ROWS, 0), expo, 0.0)
                elif row < WINDOW:
                    expo = expo * jnp.where(first > row, 0.0, 1.0)
                else:
                    expo = jnp.where(s.gap[...] <= 0, expo, 0.0)
                total += jnp.sum(expo.reshape(-1, 8, shape[1]), axis=0)
                along += jnp.sum((expo * d_probs).reshape(-1, 8, shape[1]), axis=0)
                at = slice(row, row + QUERY_ROWS)
                s.expo[slot, at] = expo.astype(jnp.bfloat16)
                s.slope[slot, at] = expo * (1.0 - bent * bent)
                s.d_probs[slot, at] = d_probs
        inverse = 1.0 / jnp.sum(total, axis=0, keepdims=True)
        delta = jnp.sum(along, axis=0, keepdims=True) * inverse
        column = jnp.transpose(jnp.broadcast_to(inverse, shape))
        return inverse, delta, column

    def gradients(head, i, slot, inverse, delta, column):
        query = (rows_of(s.query, head, i).astype(jnp.float32) * (column * SCALE)).astype(jnp.bfloat16)
        grad = (rows_of(output_grad, head, i).astype(jnp.float32) * column).astype(jnp.bfloat16)
        grad_query = jnp.zeros((shape[1], HEAD_SIZE), jnp.float32)
        for tile in range(0, span, KEY_TILE):
            rows = slice(tile, tile + KEY_TILE)
            d_raw = (s.slope[slot, rows] * (s.d_probs[slot, rows] - delta)).astype(jnp.bfloat16)
            at = slice(i * QUERY_ROWS + tile, i * QUERY_ROWS + tile + KEY_TILE)
            s.sums[head, at, :HEAD_SIZE] += dot(d_raw, query, 1, 0)
            s.sums[head, at, HEAD_SIZE:] += dot(s.expo[slot, rows], grad, 1, 0)
            grad_query += dot(d_raw, seen_by(head, i, tile, 0), 0, 0)
        grad_query = (grad_query * (column * SCALE)).astype(jnp.bfloat16)
        for g, lanes in enumerate(lanes_of(head)):
            s.grads[i * QUERY_ROWS : (i + 1) * QUERY_ROWS, lanes] = grad_query[
                g * QUERY_ROWS : (g + 1) * QUERY_ROWS
            ]

    pieces = [(piece, QUERY_ROWS) for piece in range(count - 1)] + [(count - 1, WINDOW - late)]
    steps = [(head, i) for i in range(count) for head in range(kv_heads)]
    ready = scores(*steps[0], 0)
    for k, (head, i) in enumerate(steps):
        now = ready
        if k + 1 < len(steps):
            ready = scores(*steps[k + 1], (k + 1) % 2)
        gradients(head, i, k % 2, *now)
        if i + 1 == count:
            halo(head, 0, QUERY_ROWS).wait_recv()
            s.sums[head, local:WINDOW] += s.arriving[head, :reach].astype(jnp.float32)
        send_back(head, *pieces[i])
        sends.append((halo(head, *pieces[i]), None))
    owners = first_owners(n)
    pick(s.picked_first, s.grads, owners, slice(0, query_cols), rows)
    for head in range(kv_heads):
        for piece in pieces[1:]:
            halo(head, *piece).wait_recv()
    columns = [
        (head, side, query_cols + side * key_cols + head * HEAD_SIZE)
        for head in range(kv_heads)
        for side in range(2)
    ]
    for head, side, column in columns:
        lanes = slice(side * HEAD_SIZE, (side + 1) * HEAD_SIZE)
        for i, owner in enumerate(owners):
            own = pl.ds(pl.multiple_of(WINDOW + owner * rows, rows), rows)
            far = pl.ds(pl.multiple_of(reach + owner * rows, rows), rows)
            value = s.sums[head, own, lanes] + s.arriving[head, far, lanes].astype(jnp.float32)
            s.picked_first[i * rows : (i + 1) * rows, column : column + HEAD_SIZE] = value.astype(
                jnp.bfloat16
            )

    def rest():
        for head, side, column in columns:
            lanes = slice(side * HEAD_SIZE, (side + 1) * HEAD_SIZE)
            value = s.sums[head, WINDOW:, lanes] + s.arriving[head, reach:, lanes].astype(jnp.float32)
            s.grads[:, column : column + HEAD_SIZE] = value.astype(jnp.bfloat16)

    return sends, rest


def first_owners(n):
    place = ring_place(lax.axis_index("tp"), n)
    steps = (n // 2, n // 2 - 1, 1 - n // 2)
    return [ring_device(place + step, n) for step in steps]


def later_owners(n):
    place = ring_place(lax.axis_index("tp"), n)
    steps = [step * hop for hop in range(n // 2 - 2, 0, -1) for step in (1, -1)]
    return [ring_device(place + step, n) for step in steps + [0]]


def pick(target, source, owners, lanes, rows):
    for i, owner in enumerate(owners):
        target[i * rows : (i + 1) * rows, lanes] = source[rows_at(owner, rows), lanes]


def products(total, picked, s, piece):
    count, width = total.shape[1:]
    for j in range(0, width, TILE):
        at = pl.ds(pl.multiple_of(piece * width + j, TILE), TILE)
        total[piece, :, j : j + TILE] = dot(picked[:count], s.held[at], 1, 1)


def scatter_phase(n, ring, tokens, gain, out, rest, s):
    rows, width = tokens.shape
    last = n // 2
    half = PIECES // 2
    size = width // PIECES
    cols = s.grads.shape[1]
    far = [list(range(half)), list(range(half, PIECES))]

    def sender(direction, hop, piece):
        return remote(
            s.outgoing.at[direction, hop - 1, piece],
            s.incoming.at[direction, hop - 1, piece],
            s.scatter_send.at[direction, hop - 1, piece],
            s.scatter_recv.at[direction, hop - 1, piece],
            ring[direction],
        )

    def bundle(direction, hop, side):
        part = pl.ds(side * half, half)
        return remote(
            s.outgoing.at[direction, hop - 1, part],
            s.incoming.at[direction, hop - 1, part],
            s.scatter_send.at[direction, hop - 1, side * half],
            s.scatter_recv.at[direction, hop - 1, side * half],
            ring[direction],
        )

    def parcels(direction, hop, side):
        if hop == last or (hop == last - 1 and side != direction):
            return [sender(direction, hop, piece) for piece in far[side]]
        return [bundle(direction, hop, side)]

    def give(direction, hop, piece, value):
        s.outgoing[direction, hop - 1, piece] = value.astype(jnp.bfloat16)
        sender(direction, hop, piece).start()

    def arrive(direction, hop, side):
        for copy in parcels(direction, hop, side):
            copy.wait_recv()

    def relay(direction, hop, side, source, block):
        arrive(direction, hop + 1, side)
        for piece in far[side]:
            value = source[piece, block : block + rows]
            value += s.incoming[direction, hop, piece].astype(jnp.float32)
            s.outgoing[direction, hop - 1, piece] = value.astype(jnp.bfloat16)
        bundle(direction, hop, side).start()

    def first_pair(k, carry):
        for direction in range(2):
            piece = direction * half + k
            products(s.first, s.picked_first, s, piece)
            other = 1 - direction
            block = (1 + other) * rows
            give(direction, last, piece, s.first[piece, :rows])
            give(other, last - 1, piece, s.first[piece, block : block + rows])
        return carry

    lax.fori_loop(0, half, first_pair, 0)
    owners = later_owners(n)
    rest()
    pick(s.picked_later, s.grads, owners, slice(0, cols), rows)

    def later_sums(piece, carry):
        products(s.later, s.picked_later, s, piece)
        return carry

    lax.fori_loop(0, PIECES, later_sums, 0)
    values = tokens[...].astype(jnp.float32)
    scale = lax.rsqrt(jnp.mean(values * values, axis=1, keepdims=True) + EPS)
    s.unit[...] = values * scale

    for direction in range(2):
        relay(direction, last - 1, direction, s.first, (1 + direction) * rows)
    for hop in range(last - 2, 0, -1):
        for turn in range(2):
            for direction in range(2):
                side = direction if turn else 1 - direction
                block = (2 * (last - 2 - hop) + direction) * rows
                relay(direction, hop, side, s.later, block)
    along = jnp.zeros((rows, HEAD_SIZE), jnp.float32)
    block = 2 * (last - 2) * rows
    for direction in range(2):
        side = 1 - direction
        arrive(direction, 1, side)
        for piece in far[side]:
            s.later[piece, block : block + rows] += s.incoming[direction, 0, piece].astype(jnp.float32)
    for direction in range(2):
        arrive(direction, 1, direction)
        for piece in far[direction]:
            at = slice(piece * size, (piece + 1) * size)
            value = s.later[piece, block : block + rows]
            value += s.incoming[direction, 0, piece].astype(jnp.float32)
            upper = value * gain[:, at]
            s.upper[:, at] = upper
            product = upper * s.unit[:, at]
            for j in range(0, size, HEAD_SIZE):
                along += product[:, j : j + HEAD_SIZE]
    mean = jnp.sum(along, axis=1, keepdims=True) * (1.0 / width)
    for piece in range(PIECES):
        at = slice(piece * size, (piece + 1) * size)
        out[:, at] = (scale * (s.upper[:, at] - s.unit[:, at] * mean)).astype(jnp.bfloat16)
    return [
        copy
        for hop in range(last, 0, -1)
        for direction in range(2)
        for side in range(2)
        if hop < last or side == direction
        for copy in parcels(direction, hop, side)
    ]


def kernel(names, n, seqs, tokens_ref, gain_ref, grad_ref, wq, wk, wv, out, *scratch):
    s = types.SimpleNamespace(**dict(zip(names, scratch)))
    place = ring_place(lax.axis_index("tp"), n)
    block = lax.axis_index("seq")
    ring = [{"tp": ring_device(place + step, n)} for step in (1, -1)]
    onward = [{"seq": (block + step) % seqs} for step in (1, 2)]
    backward = [{"seq": (block + seqs - step) % seqs} for step in (1, 2)]
    greet(ring + onward + backward)
    tokens = s.tokens
    load = pltpu.make_async_copy(tokens_ref, tokens, s.load_sems.at[3])
    loads = load_weights((wq, wk, wv), s.held, s.load_sems)
    loads.append(pltpu.make_async_copy(gain_ref, s.gain_flat, s.load_sems.at[4]))
    loads.append(pltpu.make_async_copy(grad_ref, s.output_grad, s.load_sems.at[5]))
    for copy in [load] + loads:
        copy.start()
    load.wait()
    hear(ring + onward + backward)
    sends = gather_phase(n, ring, onward, tokens, s.gain, loads, s)
    halos, rest = attention_phase(n, tokens.shape[0], backward[0], s.output_grad, s)
    sends += halos
    sends += [(copy, None) for copy in scatter_phase(n, ring, tokens, s.gain, out, rest, s)]
    for copy, needed in sends:
        when(needed, copy.wait_send)


def on_device(tokens, norm_gain, query_weight, key_matrix, value_matrix, output_grad):
    n = lax.axis_size("tp")
    rows, width = tokens.shape
    local, query_cols = output_grad.shape
    key_cols = key_matrix.shape[1]
    cols = query_cols + 2 * key_cols
    kv_heads = key_cols // HEAD_SIZE
    groups = query_cols // key_cols
    low, full = jnp.bfloat16, jnp.float32
    hops = pltpu.SemaphoreType.DMA((2, n // 2, 2))
    pieces = pltpu.SemaphoreType.DMA((2, n // 2, PIECES))
    blocks = pltpu.SemaphoreType.DMA((2, n + 3))
    heads = pltpu.SemaphoreType.DMA((kv_heads, local // QUERY_ROWS))
    scratch = dict(
        tokens=pltpu.VMEM((rows, width), low),
        output_grad=pltpu.VMEM((local, query_cols), low),
        gain_flat=pltpu.VMEM((width,), full),
        gain=pltpu.VMEM((1, width), full),
        gathered=pltpu.VMEM((n, rows, width), low),
        held=pltpu.VMEM((width, cols), low),
        normed=pltpu.VMEM((2 * rows, width), low),
        query=pltpu.VMEM((local, query_cols), low),
        pairs=pltpu.VMEM((3 * local, 2 * key_cols), low),
        gap=pltpu.VMEM((QUERY_ROWS, groups * QUERY_ROWS), jnp.int32),
        expo=pltpu.VMEM((2, WINDOW + QUERY_ROWS, groups * QUERY_ROWS), low),
        slope=pltpu.VMEM((2, WINDOW + QUERY_ROWS, groups * QUERY_ROWS), full),
        d_probs=pltpu.VMEM((2, WINDOW + QUERY_ROWS, groups * QUERY_ROWS), full),
        sums=pltpu.VMEM((kv_heads, WINDOW + local, 2 * HEAD_SIZE), full),
        leaving=pltpu.VMEM((kv_heads, WINDOW, 2 * HEAD_SIZE), low),
        arriving=pltpu.VMEM((kv_heads, WINDOW, 2 * HEAD_SIZE), low),
        grads=pltpu.VMEM((local, cols), low),
        outgoing=pltpu.VMEM((2, n // 2, PIECES, rows, width // PIECES), low),
        incoming=pltpu.VMEM((2, n // 2, PIECES, rows, width // PIECES), low),
        picked_first=pltpu.VMEM((3 * rows, cols), low),
        picked_later=pltpu.VMEM(((n - 3) * rows, cols), low),
        first=pltpu.VMEM((PIECES, 3 * rows, width // PIECES), full),
        later=pltpu.VMEM((PIECES, (n - 3) * rows, width // PIECES), full),
        unit=pltpu.VMEM((rows, width), full),
        upper=pltpu.VMEM((rows, width), full),
        gather_send=hops,
        gather_recv=hops,
        halo_send=blocks,
        halo_recv=blocks,
        back_send=heads,
        back_recv=heads,
        scatter_send=pieces,
        scatter_recv=pieces,
        load_sems=pltpu.SemaphoreType.DMA((6,)),
    )
    vmem = pl.BlockSpec(memory_space=pltpu.VMEM)
    hbm = pl.BlockSpec(memory_space=pl.ANY)
    return pl.pallas_call(
        functools.partial(kernel, tuple(scratch), n, lax.axis_size("seq")),
        out_shape=pltpu.VMEM((rows, width), low),
        in_specs=[hbm] * 6,
        out_specs=vmem,
        scratch_shapes=list(scratch.values()),
        compiler_params=pltpu.CompilerParams(
            collective_id=0, has_side_effects=True, vmem_limit_bytes=VMEM_BYTES
        ),
        name="attention_backward",
    )(tokens, norm_gain, output_grad, query_weight, key_matrix, value_matrix)


def solution(mesh):
    return jax.shard_map(
        on_device,
        mesh=mesh,
        in_specs=(
            P(("seq", "tp"), None),
            P(),
            P(None, "tp"),
            P(None, "tp"),
            P(None, "tp"),
            P("seq", "tp"),
        ),
        out_specs=P(("seq", "tp"), None),
        check_vma=False,
    )
```

```python
import functools
import types

import jax
import jax.numpy as jnp
from jax import lax
from jax.experimental import pallas as pl
from jax.experimental.pallas import tpu as pltpu
from jax.sharding import PartitionSpec as P

HEAD_SIZE = 128
WINDOW = 640


SCALE = 1.0 / 12.0
CAP = 50.0
EPS = 1e-06
VMEM_BYTES = 60 * 1024 * 1024
QUERY_ROWS = 128
KEY_TILE = 256
PIECES = 6
LOG2E = 1.4426950408889634
TILE = 256


def ring_place(index, n):
    odd = index % 2
    return (1 - odd) * (index // 2) + odd * (n - 1 - index // 2)


def ring_device(place, n):
    place = (place + n) % n
    late = place // (n // 2)
    return (1 - late) * 2 * place + late * (2 * (n - 1 - place) + 1)


def chunks_of(direction, hop, last):
    return (direction, 1 - direction) if hop < last else (direction,)


def greet(neighbours):
    barrier = pltpu.get_barrier_semaphore()
    for neighbour in neighbours:
        pl.semaphore_signal(
            barrier, inc=1, device_id=neighbour, device_id_type=pl.DeviceIdType.MESH
        )


def hear(neighbours):
    pl.semaphore_wait(pltpu.get_barrier_semaphore(), len(neighbours))


def when(needed, act):
    if needed is None:
        act()
    else:
        pl.when(needed)(act)


def remote(source, target, send_sem, recv_sem, device):
    return pltpu.make_async_remote_copy(
        src_ref=source,
        dst_ref=target,
        send_sem=send_sem,
        recv_sem=recv_sem,
        device_id=device,
        device_id_type=pl.DeviceIdType.MESH,
    )


def load_weights(weights, held, sems):
    copies = []
    start = 0
    for i, weight in enumerate(weights):
        cols = weight.shape[1]
        copies.append(
            pltpu.make_async_copy(weight, held.at[:, start : start + cols], sems.at[i])
        )
        start += cols
    return copies


def rows_at(index, count):
    return pl.ds(pl.multiple_of(index * count, count), count)


def gather_phase(n, ring, onward, tokens, gain, loads, s):
    rows, _ = tokens.shape
    local = n * rows
    half = rows // 2
    quarter = half // 2
    last = n // 2
    query_cols = s.query.shape[1]
    pair_cols = s.pairs.shape[1]
    me = lax.axis_index("tp")
    place = ring_place(me, n)
    sends = []
    halos = []

    def sender(direction, hop, chunk):
        step = -(hop - 1) if direction == 0 else hop - 1
        owner = ring_device(place + step, n)
        part = pl.ds(chunk * half, half)
        return remote(
            tokens.at[part] if hop == 1 else s.gathered.at[owner, part],
            s.gathered.at[owner, part],
            s.gather_send.at[direction, hop - 1, chunk],
            s.gather_recv.at[direction, hop - 1, chunk],
            ring[direction],
        )

    def last_sender(direction, stage):
        owner = ring_device(place + (1 - last if direction == 0 else last - 1), n)
        part = pl.ds(direction * half + stage * quarter, quarter)
        return remote(
            s.gathered.at[owner, part],
            s.gathered.at[owner, part],
            s.gather_send.at[direction, last - 1, stage],
            s.gather_recv.at[direction, last - 1, stage],
            ring[direction],
        )

    def normalize(pieces, at):
        for block, _, size in pieces:
            values = block[...].astype(jnp.float32)
            scale = lax.rsqrt(jnp.mean(values * values, axis=1, keepdims=True) + EPS)
            s.normed[at : at + size] = (values * scale * gain[...]).astype(jnp.bfloat16)
            at += size

    def columns(pieces, at, tiles, target, base, first):
        count = sum(size for _, _, size in pieces)

        def write(j, carry):
            product = jnp.dot(
                s.normed[at : at + count],
                s.held[:, pl.ds(pl.multiple_of(first + j * TILE, TILE), TILE)],
                preferred_element_type=jnp.float32,
            ).astype(jnp.bfloat16)
            done = 0
            for _, row, size in pieces:
                to = pl.ds(pl.multiple_of(base + row, size), size)
                target[to, rows_at(j, TILE)] = product[done : done + size]
                done += size
            return carry

        lax.fori_loop(0, tiles, write, 0)

    def pairs(pieces, at):
        columns(pieces, at, pair_cols // TILE, s.pairs, 2 * local, query_cols)
        for _, row, size in pieces:
            for back in range(2):
                copy = remote(
                    s.pairs.at[pl.ds(pl.multiple_of(2 * local + row, size), size)],
                    s.pairs.at[pl.ds(pl.multiple_of((1 - back) * local + row, size), size)],
                    s.halo_send.at[back, len(halos) // 2],
                    s.halo_recv.at[back, len(halos) // 2],
                    onward[back],
                )
                needed = row + size > 2 * local - WINDOW if back else None
                halos.append((copy, needed))
                when(needed, copy.start)

    def queries(pieces, at):
        columns(pieces, at, query_cols // TILE, s.query, 0, 0)

    def project(sources):
        pieces = [(block, owner * rows, rows) for block, owner in sources]
        normalize(pieces, 0)
        pairs(pieces, 0)
        queries(pieces, 0)

    for position in range(2):
        for direction in range(2):
            order = chunks_of(direction, 1, last)
            if position < len(order):
                sends.append(sender(direction, 1, order[position]))
                sends[-1].start()
    for copy in loads:
        copy.wait()
    gain[...] = s.gain_flat[...].reshape(gain.shape)
    project([(tokens, me)])
    prepare_attention(s)
    for hop in range(1, last):
        for position in range(2):
            for direction in range(2):
                chunk = chunks_of(direction, hop, last)[position]
                sender(direction, hop, chunk).wait_recv()
                if hop + 1 < last:
                    sends.append(sender(direction, hop + 1, chunk))
                    sends[-1].start()
                elif chunk == direction:
                    for stage in range(2):
                        sends.append(last_sender(direction, stage))
                        sends[-1].start()
        owners = [ring_device(place - hop, n), ring_device(place + hop, n)]
        project([(s.gathered.at[owner], owner) for owner in owners])
    owner = ring_device(place + last, n)
    pieces = []
    for stage in range(2):
        for direction in range(2):
            last_sender(direction, stage).wait_recv()
            first = direction * half + stage * quarter
            block = s.gathered.at[owner, first : first + quarter]
            pieces.append((block, owner * rows + first, quarter))
        normalize(pieces[2 * stage :], stage * half)
        pairs(pieces[2 * stage :], stage * half)
    queries(pieces, 0)
    for copy, needed in halos:
        when(needed, copy.wait_recv)
    return [(copy, None) for copy in sends] + halos


def dot(lhs, rhs, left, right):
    return lax.dot_general(
        lhs, rhs, (((left,), (right,)), ((), ())), preferred_element_type=jnp.float32
    )


def prepare_attention(s):
    shape = s.gap.shape
    s.gap[...] = lax.broadcasted_iota(jnp.int32, shape, 0) - (
        lax.broadcasted_iota(jnp.int32, shape, 1) % QUERY_ROWS
    )
    s.sums[...] = jnp.zeros_like(s.sums)


def attention_phase(n, rows, backward, output_grad, s):
    local, query_cols = s.query.shape
    key_cols = s.pairs.shape[1] // 2
    kv_heads = key_cols // HEAD_SIZE
    groups = query_cols // key_cols
    reach = WINDOW - local
    span = WINDOW + QUERY_ROWS
    start = 2 * local - WINDOW
    anchor = lax.axis_index("seq") * local
    shape = s.gap.shape
    sends = []

    count = local // QUERY_ROWS
    late = (count - 1) * QUERY_ROWS

    def halo(head, piece, rows):
        part = pl.ds(pl.multiple_of(piece * QUERY_ROWS, QUERY_ROWS), rows)
        return remote(
            s.leaving.at[head, part],
            s.arriving.at[head, part],
            s.back_send.at[head, piece],
            s.back_recv.at[head, piece],
            backward,
        )

    def send_back(head, piece, rows):
        part = pl.ds(pl.multiple_of(piece * QUERY_ROWS, QUERY_ROWS), rows)
        s.leaving[head, part] = s.sums[head, part].astype(jnp.bfloat16)
        halo(head, piece, rows).start()

    def lanes_of(head):
        return [
            slice((head * groups + g) * HEAD_SIZE, (head * groups + g + 1) * HEAD_SIZE)
            for g in range(groups)
        ]

    def rows_of(ref, head, i):
        own = slice(i * QUERY_ROWS, (i + 1) * QUERY_ROWS)
        return jnp.concatenate([ref[own, lanes] for lanes in lanes_of(head)], axis=0)

    def seen_by(head, i, tile, base):
        rows = slice(start + i * QUERY_ROWS + tile, start + i * QUERY_ROWS + tile + KEY_TILE)
        return s.pairs[rows, base + head * HEAD_SIZE : base + (head + 1) * HEAD_SIZE]

    def scores(head, i, slot):
        query = rows_of(s.query, head, i)
        grad = rows_of(output_grad, head, i)
        first = WINDOW - anchor - i * QUERY_ROWS
        total = jnp.zeros((8, shape[1]), jnp.float32)
        along = jnp.zeros((8, shape[1]), jnp.float32)
        for tile in range(0, span, KEY_TILE):
            bent_tile = jnp.tanh(dot(seen_by(head, i, tile, 0), query, 1, 1) * (SCALE / CAP))
            d_tile = dot(seen_by(head, i, tile, key_cols), grad, 1, 1)
            for part in range(0, KEY_TILE, QUERY_ROWS):
                row = tile + part
                bent = bent_tile[part : part + QUERY_ROWS]
                d_probs = d_tile[part : part + QUERY_ROWS]
                expo = jnp.exp2(bent * (CAP * LOG2E))
                if row == 0:
                    expo = jnp.where(s.gap[...] > jnp.where(first > 0, QUERY_ROWS, 0), expo, 0.0)
                elif row < WINDOW:
                    expo = expo * jnp.where(first > row, 0.0, 1.0)
                else:
                    expo = jnp.where(s.gap[...] <= 0, expo, 0.0)
                total += jnp.sum(expo.reshape(-1, 8, shape[1]), axis=0)
                along += jnp.sum((expo * d_probs).reshape(-1, 8, shape[1]), axis=0)
                at = slice(row, row + QUERY_ROWS)
                s.expo[slot, at] = expo.astype(jnp.bfloat16)
                s.slope[slot, at] = expo * (1.0 - bent * bent)
                s.d_probs[slot, at] = d_probs
        inverse = 1.0 / jnp.sum(total, axis=0, keepdims=True)
        delta = jnp.sum(along, axis=0, keepdims=True) * inverse
        column = jnp.transpose(jnp.broadcast_to(inverse, shape))
        return inverse, delta, column

    def gradients(head, i, slot, inverse, delta, column):
        query = (rows_of(s.query, head, i).astype(jnp.float32) * (column * SCALE)).astype(jnp.bfloat16)
        grad = (rows_of(output_grad, head, i).astype(jnp.float32) * column).astype(jnp.bfloat16)
        grad_query = jnp.zeros((shape[1], HEAD_SIZE), jnp.float32)
        for tile in range(0, span, KEY_TILE):
            rows = slice(tile, tile + KEY_TILE)
            d_raw = (s.slope[slot, rows] * (s.d_probs[slot, rows] - delta)).astype(jnp.bfloat16)
            at = slice(i * QUERY_ROWS + tile, i * QUERY_ROWS + tile + KEY_TILE)
            s.sums[head, at, :HEAD_SIZE] += dot(d_raw, query, 1, 0)
            s.sums[head, at, HEAD_SIZE:] += dot(s.expo[slot, rows], grad, 1, 0)
            grad_query += dot(d_raw, seen_by(head, i, tile, 0), 0, 0)
        grad_query = (grad_query * (column * SCALE)).astype(jnp.bfloat16)
        for g, lanes in enumerate(lanes_of(head)):
            s.grads[i * QUERY_ROWS : (i + 1) * QUERY_ROWS, lanes] = grad_query[
                g * QUERY_ROWS : (g + 1) * QUERY_ROWS
            ]

    pieces = [(piece, QUERY_ROWS) for piece in range(count - 1)] + [(count - 1, WINDOW - late)]
    steps = [(head, i) for i in range(count) for head in range(kv_heads)]
    ready = scores(*steps[0], 0)
    for k, (head, i) in enumerate(steps):
        now = ready
        if k + 1 < len(steps):
            ready = scores(*steps[k + 1], (k + 1) % 2)
        gradients(head, i, k % 2, *now)
        if i + 1 == count:
            halo(head, 0, QUERY_ROWS).wait_recv()
            s.sums[head, local:WINDOW] += s.arriving[head, :reach].astype(jnp.float32)
        send_back(head, *pieces[i])
        sends.append((halo(head, *pieces[i]), None))
    owners = first_owners(n)
    pick(s.picked_first, s.grads, owners, slice(0, query_cols), rows)
    for head in range(kv_heads):
        for piece in pieces[1:]:
            halo(head, *piece).wait_recv()
    columns = [
        (head, side, query_cols + side * key_cols + head * HEAD_SIZE)
        for head in range(kv_heads)
        for side in range(2)
    ]
    for head, side, column in columns:
        lanes = slice(side * HEAD_SIZE, (side + 1) * HEAD_SIZE)
        for i, owner in enumerate(owners):
            own = pl.ds(pl.multiple_of(WINDOW + owner * rows, rows), rows)
            far = pl.ds(pl.multiple_of(reach + owner * rows, rows), rows)
            value = s.sums[head, own, lanes] + s.arriving[head, far, lanes].astype(jnp.float32)
            s.picked_first[i * rows : (i + 1) * rows, column : column + HEAD_SIZE] = value.astype(
                jnp.bfloat16
            )

    def rest():
        for head, side, column in columns:
            lanes = slice(side * HEAD_SIZE, (side + 1) * HEAD_SIZE)
            value = s.sums[head, WINDOW:, lanes] + s.arriving[head, reach:, lanes].astype(jnp.float32)
            s.grads[:, column : column + HEAD_SIZE] = value.astype(jnp.bfloat16)

    return sends, rest


def first_owners(n):
    place = ring_place(lax.axis_index("tp"), n)
    steps = (n // 2, n // 2 - 1, 1 - n // 2)
    return [ring_device(place + step, n) for step in steps]


def later_owners(n):
    place = ring_place(lax.axis_index("tp"), n)
    steps = [step * hop for hop in range(n // 2 - 2, 0, -1) for step in (1, -1)]
    return [ring_device(place + step, n) for step in steps + [0]]


def pick(target, source, owners, lanes, rows):
    for i, owner in enumerate(owners):
        target[i * rows : (i + 1) * rows, lanes] = source[rows_at(owner, rows), lanes]


def products(total, picked, s, piece):
    count, width = total.shape[1:]
    for j in range(0, width, TILE):
        at = pl.ds(pl.multiple_of(piece * width + j, TILE), TILE)
        total[piece, :, j : j + TILE] = dot(picked[:count], s.held[at], 1, 1)


def scatter_phase(n, ring, tokens, gain, out, rest, s):
    rows, width = tokens.shape
    last = n // 2
    half = PIECES // 2
    size = width // PIECES
    cols = s.grads.shape[1]
    far = [list(range(half)), list(range(half, PIECES))]

    def sender(direction, hop, piece):
        return remote(
            s.outgoing.at[direction, hop - 1, piece],
            s.incoming.at[direction, hop - 1, piece],
            s.scatter_send.at[direction, hop - 1, piece],
            s.scatter_recv.at[direction, hop - 1, piece],
            ring[direction],
        )

    def bundle(direction, hop, side):
        part = pl.ds(side * half, half)
        return remote(
            s.outgoing.at[direction, hop - 1, part],
            s.incoming.at[direction, hop - 1, part],
            s.scatter_send.at[direction, hop - 1, side * half],
            s.scatter_recv.at[direction, hop - 1, side * half],
            ring[direction],
        )

    def parcels(direction, hop, side):
        single = (hop == 1) if side == direction else (hop == last - 1)
        if hop == last or single:
            return [sender(direction, hop, piece) for piece in far[side]]
        return [bundle(direction, hop, side)]

    def give(direction, hop, piece, value):
        s.outgoing[direction, hop - 1, piece] = value.astype(jnp.bfloat16)
        sender(direction, hop, piece).start()

    def arrive(direction, hop, side):
        for copy in parcels(direction, hop, side):
            copy.wait_recv()

    def relay(direction, hop, side, source, block):
        arrive(direction, hop + 1, side)
        for piece in far[side]:
            value = source[piece, block : block + rows]
            value += s.incoming[direction, hop, piece].astype(jnp.float32)
            s.outgoing[direction, hop - 1, piece] = value.astype(jnp.bfloat16)
        for copy in parcels(direction, hop, side):
            copy.start()

    def first_pair(k, carry):
        for direction in range(2):
            piece = direction * half + k
            products(s.first, s.picked_first, s, piece)
            other = 1 - direction
            block = (1 + other) * rows
            give(direction, last, piece, s.first[piece, :rows])
            give(other, last - 1, piece, s.first[piece, block : block + rows])
        return carry

    lax.fori_loop(0, half, first_pair, 0)
    owners = later_owners(n)
    rest()
    pick(s.picked_later, s.grads, owners, slice(0, cols), rows)

    def later_sums(piece, carry):
        products(s.later, s.picked_later, s, piece)
        return carry

    lax.fori_loop(0, PIECES, later_sums, 0)
    values = tokens[...].astype(jnp.float32)
    scale = lax.rsqrt(jnp.mean(values * values, axis=1, keepdims=True) + EPS)
    s.unit[...] = values * scale

    for direction in range(2):
        relay(direction, last - 1, direction, s.first, (1 + direction) * rows)
    for hop in range(last - 2, 0, -1):
        for turn in range(2):
            for direction in range(2):
                side = direction if turn else 1 - direction
                block = (2 * (last - 2 - hop) + direction) * rows
                relay(direction, hop, side, s.later, block)
    along = jnp.zeros((rows, HEAD_SIZE), jnp.float32)
    block = 2 * (last - 2) * rows
    for direction in range(2):
        side = 1 - direction
        arrive(direction, 1, side)
        for piece in far[side]:
            s.later[piece, block : block + rows] += s.incoming[direction, 0, piece].astype(jnp.float32)
    for k in range(half):
        for direction in range(2):
            piece = far[direction][k]
            sender(direction, 1, piece).wait_recv()
            at = slice(piece * size, (piece + 1) * size)
            value = s.later[piece, block : block + rows]
            value += s.incoming[direction, 0, piece].astype(jnp.float32)
            upper = value * gain[:, at]
            s.upper[:, at] = upper
            product = upper * s.unit[:, at]
            for j in range(0, size, HEAD_SIZE):
                along += product[:, j : j + HEAD_SIZE]
    mean = jnp.sum(along, axis=1, keepdims=True) * (1.0 / width)
    for piece in range(PIECES):
        at = slice(piece * size, (piece + 1) * size)
        out[:, at] = (scale * (s.upper[:, at] - s.unit[:, at] * mean)).astype(jnp.bfloat16)
    return [
        copy
        for hop in range(last, 0, -1)
        for direction in range(2)
        for side in range(2)
        if hop < last or side == direction
        for copy in parcels(direction, hop, side)
    ]


def kernel(names, n, seqs, tokens_ref, gain_ref, grad_ref, wq, wk, wv, out, *scratch):
    s = types.SimpleNamespace(**dict(zip(names, scratch)))
    place = ring_place(lax.axis_index("tp"), n)
    block = lax.axis_index("seq")
    ring = [{"tp": ring_device(place + step, n)} for step in (1, -1)]
    onward = [{"seq": (block + step) % seqs} for step in (1, 2)]
    backward = [{"seq": (block + seqs - step) % seqs} for step in (1, 2)]
    greet(ring + onward + backward)
    tokens = s.tokens
    load = pltpu.make_async_copy(tokens_ref, tokens, s.load_sems.at[3])
    loads = load_weights((wq, wk, wv), s.held, s.load_sems)
    loads.append(pltpu.make_async_copy(gain_ref, s.gain_flat, s.load_sems.at[4]))
    loads.append(pltpu.make_async_copy(grad_ref, s.output_grad, s.load_sems.at[5]))
    for copy in [load] + loads:
        copy.start()
    load.wait()
    hear(ring + onward + backward)
    sends = gather_phase(n, ring, onward, tokens, s.gain, loads, s)
    halos, rest = attention_phase(n, tokens.shape[0], backward[0], s.output_grad, s)
    sends += halos
    sends += [(copy, None) for copy in scatter_phase(n, ring, tokens, s.gain, out, rest, s)]
    for copy, needed in sends:
        when(needed, copy.wait_send)


def on_device(tokens, norm_gain, query_weight, key_matrix, value_matrix, output_grad):
    n = lax.axis_size("tp")
    rows, width = tokens.shape
    local, query_cols = output_grad.shape
    key_cols = key_matrix.shape[1]
    cols = query_cols + 2 * key_cols
    kv_heads = key_cols // HEAD_SIZE
    groups = query_cols // key_cols
    low, full = jnp.bfloat16, jnp.float32
    hops = pltpu.SemaphoreType.DMA((2, n // 2, 2))
    pieces = pltpu.SemaphoreType.DMA((2, n // 2, PIECES))
    blocks = pltpu.SemaphoreType.DMA((2, n + 3))
    heads = pltpu.SemaphoreType.DMA((kv_heads, local // QUERY_ROWS))
    scratch = dict(
        tokens=pltpu.VMEM((rows, width), low),
        output_grad=pltpu.VMEM((local, query_cols), low),
        gain_flat=pltpu.VMEM((width,), full),
        gain=pltpu.VMEM((1, width), full),
        gathered=pltpu.VMEM((n, rows, width), low),
        held=pltpu.VMEM((width, cols), low),
        normed=pltpu.VMEM((2 * rows, width), low),
        query=pltpu.VMEM((local, query_cols), low),
        pairs=pltpu.VMEM((3 * local, 2 * key_cols), low),
        gap=pltpu.VMEM((QUERY_ROWS, groups * QUERY_ROWS), jnp.int32),
        expo=pltpu.VMEM((2, WINDOW + QUERY_ROWS, groups * QUERY_ROWS), low),
        slope=pltpu.VMEM((2, WINDOW + QUERY_ROWS, groups * QUERY_ROWS), full),
        d_probs=pltpu.VMEM((2, WINDOW + QUERY_ROWS, groups * QUERY_ROWS), full),
        sums=pltpu.VMEM((kv_heads, WINDOW + local, 2 * HEAD_SIZE), full),
        leaving=pltpu.VMEM((kv_heads, WINDOW, 2 * HEAD_SIZE), low),
        arriving=pltpu.VMEM((kv_heads, WINDOW, 2 * HEAD_SIZE), low),
        grads=pltpu.VMEM((local, cols), low),
        outgoing=pltpu.VMEM((2, n // 2, PIECES, rows, width // PIECES), low),
        incoming=pltpu.VMEM((2, n // 2, PIECES, rows, width // PIECES), low),
        picked_first=pltpu.VMEM((3 * rows, cols), low),
        picked_later=pltpu.VMEM(((n - 3) * rows, cols), low),
        first=pltpu.VMEM((PIECES, 3 * rows, width // PIECES), full),
        later=pltpu.VMEM((PIECES, (n - 3) * rows, width // PIECES), full),
        unit=pltpu.VMEM((rows, width), full),
        upper=pltpu.VMEM((rows, width), full),
        gather_send=hops,
        gather_recv=hops,
        halo_send=blocks,
        halo_recv=blocks,
        back_send=heads,
        back_recv=heads,
        scatter_send=pieces,
        scatter_recv=pieces,
        load_sems=pltpu.SemaphoreType.DMA((6,)),
    )
    vmem = pl.BlockSpec(memory_space=pltpu.VMEM)
    hbm = pl.BlockSpec(memory_space=pl.ANY)
    return pl.pallas_call(
        functools.partial(kernel, tuple(scratch), n, lax.axis_size("seq")),
        out_shape=pltpu.VMEM((rows, width), low),
        in_specs=[hbm] * 6,
        out_specs=vmem,
        scratch_shapes=list(scratch.values()),
        compiler_params=pltpu.CompilerParams(
            collective_id=0, has_side_effects=True, vmem_limit_bytes=VMEM_BYTES
        ),
        name="attention_backward",
    )(tokens, norm_gain, output_grad, query_weight, key_matrix, value_matrix)


def solution(mesh):
    return jax.shard_map(
        on_device,
        mesh=mesh,
        in_specs=(
            P(("seq", "tp"), None),
            P(),
            P(None, "tp"),
            P(None, "tp"),
            P(None, "tp"),
            P("seq", "tp"),
        ),
        out_specs=P(("seq", "tp"), None),
        check_vma=False,
    )
```
